32 devices in a mesh: replica: 16 (over z, y, core), shard: 2 (over x).
Axes of the slice: x: 2, y: 2, z: 4, core: 2. Of those that a mesh axis runs over, the one named last changes fastest.
Arguments:
- weight: bfloat16 [256, 8192], P(None, 'shard'), may hold values from -6 to 6
- momentum: float32 [16, 256, 8192], P('replica', None, 'shard'), may hold values from -6 to 6
- grad: bfloat16 [16, 256, 8192], P('replica', None, 'shard'), may hold values from -6 to 6
- positions: int32 [16, 4, 128, 32], P('replica', None, 'shard'), may hold values from 0 to 4095, as said below
Outputs:
- kept_state: float32 [16, 256, 8192], P('replica', None, 'shard')
- direction: bfloat16 [256, 8192], P(None, 'shard')
- new_weight: bfloat16 [256, 8192], replicated
The draws below stay inside these ranges and needn't reach their ends.
Inputs may be any that keep to these rules, and one draw needn't show every extreme that they name: The 32 positions of one block on one replica are distinct; replicas choose independently.
All inputs are finite; a program needn't handle non-finite values.
Results may differ from the reference program's by a relative error of at most 0.001.
Values may be sent and summed in bfloat16 or wider, within the bound.
A program may use at most 128 MiB of HBM per device.

```python
import math
import jax
import jax.numpy as jnp
from jax import lax

D = 8192
GROUP = 64
TOPK = 32
ROWS = 256
REPLICAS = 16


def draw_positions(key, part):
    shape = (REPLICAS, ROWS // GROUP, D // GROUP, GROUP * GROUP)
    scores = jax.random.randint(key, shape, 0, 1 << 18, dtype=jnp.int32) * (GROUP * GROUP)
    scores = scores + jnp.arange(GROUP * GROUP, dtype=jnp.int32)
    chosen = lax.top_k(scores, TOPK)[1]
    return chosen.astype(jnp.int32)


def block_levels(key, extent, split, smallest, top_value):
    level, own = 1.0, jax.random.fold_in(key, 6)
    for axis_at, shards_of in split:
        heights = jnp.exp(jax.random.uniform(jax.random.fold_in(own, axis_at), (shards_of,), jnp.float32, smallest / len(split), top_value / len(split)))
        level = level * jnp.repeat(heights, extent[axis_at] // shards_of).reshape([-1 if axis == axis_at else 1 for axis in range(len(extent))])
    return level


def centred(key, dims, width, bound, split=(), kind=jnp.bfloat16):
    values = jax.random.normal(key, dims, jnp.float32) * width
    if len(split) > 0:
        values = block_levels(key, dims, split, -0.22, 0.18) * values
    return jnp.clip(values, min=-bound, max=bound).astype(kind)


def setup_inputs(seed: int = 0) -> dict:
    splits = jax.random.split(jax.random.key(seed), 5)
    return {
        "weight": centred(splits[0], (ROWS, D), 1.0, 6.0, ((1, 2),)),
        "momentum": centred(splits[1], (REPLICAS, ROWS, D), 1.0, 6.0, ((0, 16), (2, 2)), jnp.float32),
        "grad": centred(splits[2], (REPLICAS, ROWS, D), 1.0, 6.0, ((0, 16), (2, 2))),
        "positions": draw_positions(jax.random.fold_in(splits[4], 71), 0),
    }


beta_decay = 0.9
step_rate = 0.02

def dct_basis():
    freq = jnp.arange(GROUP, dtype=jnp.float32)[:, None]
    cells = jnp.arange(GROUP, dtype=jnp.float32)[None, :]
    scales = jnp.where(freq == 0, math.sqrt(1.0 / GROUP), math.sqrt(2.0 / GROUP))
    return scales * jnp.cos(math.pi * (2.0 * cells + 1.0) * freq / (2.0 * GROUP))

def reference(weight, momentum, grad, positions):
    basis_table = dct_basis()
    row_blocks = ROWS // GROUP
    col_blocks = D // GROUP
    row_index = jnp.arange(row_blocks, dtype=jnp.int32)[:, None, None]
    col_index = jnp.arange(col_blocks, dtype=jnp.int32)[None, :, None]

    def scatter_coeffs(values, where):
        flat = jnp.zeros((row_blocks, col_blocks, GROUP * GROUP), jnp.float32)
        flat = flat.at[row_index, col_index, where].add(values)
        return flat.reshape(row_blocks, col_blocks, GROUP, GROUP)

    def inverse(coeff_blocks):
        dense = jnp.einsum('ai,xyab,bj->xiyj', basis_table, coeff_blocks, basis_table, precision=lax.Precision.HIGHEST)
        return dense.reshape(ROWS, D)

    def one_replica(triple):
        state, slope, where = triple
        moved = beta_decay * state + slope.astype(jnp.float32)
        blocks = moved.reshape(row_blocks, GROUP, col_blocks, GROUP)
        coeff = jnp.einsum('ai,xiyj,bj->xyab', basis_table, blocks, basis_table, precision=lax.Precision.HIGHEST)
        coeff = coeff.reshape(row_blocks, col_blocks, GROUP * GROUP)
        picked = jnp.take_along_axis(coeff, where, axis=2)
        return (moved - inverse(scatter_coeffs(picked, where)), picked)
    kept_state, picked_all = lax.map(one_replica, (momentum, grad, positions))
    values = jnp.moveaxis(picked_all, 0, 2).reshape(row_blocks, col_blocks, REPLICAS * TOPK)
    where = jnp.moveaxis(positions, 0, 2).reshape(row_blocks, col_blocks, REPLICAS * TOPK)
    smooth = jnp.tanh(inverse(scatter_coeffs(values, where)))
    direction = smooth.astype(jnp.bfloat16)
    new_weight = (weight.astype(jnp.float32) - step_rate * smooth).astype(jnp.bfloat16)
    return (kept_state, direction, new_weight)
```

```python
import functools
import math

import jax
import jax.numpy as jnp
import numpy as np
from jax import lax
from jax.experimental import pallas as pl
from jax.experimental.pallas import tpu as pltpu
from jax.sharding import PartitionSpec as P

GROUP = 64
LANES = 128
WIDE = 256
PAIR = 128

beta_decay = 0.9
step_rate = 0.02

f32, bf16 = jnp.float32, jnp.bfloat16
MESH = pl.DeviceIdType.MESH


def basis():
    k = np.arange(GROUP, dtype=np.float64)[:, None]
    i = np.arange(GROUP, dtype=np.float64)[None, :]
    scale = np.where(k == 0, math.sqrt(1.0 / GROUP), math.sqrt(2.0 / GROUP))
    return scale * np.cos(math.pi * (2.0 * i + 1.0) * k / (2.0 * GROUP))


def halves(c):
    full = np.kron(np.eye(PAIR // GROUP), c).astype(np.float32)
    high = full.astype(bf16)
    low = (full - high.astype(np.float32)).astype(bf16)
    return high, low


def left_basis(c):
    high, low = halves(c)
    return np.block([[high, high], [low, low]])


def right_basis(c):
    high, low = halves(c)
    return np.block([[high, low], [high, low]])


def split(x):
    high = x.astype(bf16)
    return high, (x - high.astype(f32)).astype(bf16)


def dot(a, b):
    return jnp.dot(a, b, preferred_element_type=f32)


def dot_t(a, b):
    return lax.dot_general(a, b, (((1,), (1,)), ((), ())), preferred_element_type=f32)


def left(m, x):
    high, low = split(x)
    parts = []
    for at in range(0, x.shape[0], PAIR):
        both = dot(m, jnp.concatenate([high[at : at + PAIR], low[at : at + PAIR]], axis=0))
        parts.append(both[:PAIR] + both[PAIR:])
    return jnp.concatenate(parts, axis=0)


def right(x, m):
    high, low = split(x)
    rows = x.shape[0]
    ats = range(0, x.shape[1], PAIR)
    both = dot(jnp.concatenate([
        jnp.concatenate([high[:, at : at + PAIR], low[:, at : at + PAIR]], axis=1) for at in ats
    ], axis=0), m)
    both = both[:, :PAIR] + both[:, PAIR:]
    return jnp.concatenate([both[i * rows : (i + 1) * rows] for i in range(len(ats))], axis=1)


def down(rows):
    return lax.broadcasted_iota(jnp.int32, (rows, LANES), 0).astype(f32)


def lane_offset(topk):
    lane = lax.broadcasted_iota(jnp.int32, (1, LANES), 1)
    return (lane // topk * GROUP).astype(f32)


def place(pos, topk):
    a = jnp.floor(pos * (1.0 / GROUP))
    return a, pos - a * GROUP + lane_offset(topk)


def own_kernel(nx, topk, mom, grad, pos, lf, rt, li, ri, kept, sent):
    lf, rt, li, ri = lf[...], rt[...], li[...], ri[...]
    moved = beta_decay * mom[0] + grad[0].astype(f32)
    coeff = right(left(lf, moved), rt)
    spots = pos[0]
    a, b = place(spots, topk)
    rows, cols = down(GROUP), down(WIDE)
    picked, own = [], []
    for x in range(nx):
        part = coeff[x * GROUP : (x + 1) * GROUP]
        at_row = rows == a[x : x + 1]
        hot_a = jnp.where(at_row, 1.0, 0.0).astype(bf16)
        hot_b = jnp.where(cols == b[x : x + 1], 1.0, 0.0).astype(bf16)
        own.append(part * dot_t(hot_a, hot_b))
        high, low = split(part)
        found = dot(jnp.concatenate([high, low], axis=0), hot_b)
        found = found[:GROUP] + found[GROUP:]
        picked.append(jnp.sum(jnp.where(at_row, found, 0.0), axis=0, keepdims=True))
    kept[0] = moved - right(left(li, jnp.concatenate(own, axis=0)), ri)
    sent[0] = jnp.concatenate(picked + [spots], axis=0)


def own_part(mom, grad, pos, topk, interpret=False):
    _, rows, width = mom.shape
    nx = rows // GROUP
    steps = width // WIDE
    whole = pl.BlockSpec((2 * PAIR, 2 * PAIR), lambda g: (0, 0))
    return pl.pallas_call(
        functools.partial(own_kernel, nx, topk),
        grid=(steps,),
        in_specs=[
            pl.BlockSpec((1, rows, WIDE), lambda g: (0, 0, g)),
            pl.BlockSpec((1, rows, WIDE), lambda g: (0, 0, g)),
            pl.BlockSpec((1, nx, LANES), lambda g: (g, 0, 0)),
            whole, whole, whole, whole,
        ],
        out_specs=[
            pl.BlockSpec((1, rows, WIDE), lambda g: (0, 0, g)),
            pl.BlockSpec((1, 2 * nx, LANES), lambda g: (g, 0, 0)),
        ],
        out_shape=[
            jax.ShapeDtypeStruct((1, rows, width), f32),
            jax.ShapeDtypeStruct((steps, 2 * nx, LANES), f32),
        ],
        interpret=interpret,
        name="own_part",
    )(
        mom, grad, pos,
        left_basis(basis()), right_basis(basis().T),
        left_basis(basis().T), right_basis(basis()),
    )


def swap_kernel(reps, shards, mine, got, send_sem, recv_sem, own_sem):
    r, s = lax.axis_index("replica"), lax.axis_index("shard")
    me = r * shards + s
    total = reps * shards
    keep = pltpu.make_async_copy(mine.at[lax.rem(r, 2)], got.at[s, r], own_sem)
    keep.start()

    def push(step):
        to = lax.rem(me + step, total)
        to_r, to_s = to // shards, lax.rem(to, shards)
        return pltpu.make_async_remote_copy(
            src_ref=mine.at[lax.rem(to_r, 2)],
            dst_ref=got.at[s, r],
            send_sem=send_sem.at[step],
            recv_sem=recv_sem.at[step],
            device_id=(to_r, to_s),
            device_id_type=MESH,
        )

    def come(step):
        of = lax.rem(me - step + total, total)
        of_r, of_s = of // shards, lax.rem(of, shards)
        return pltpu.make_async_remote_copy(
            src_ref=mine.at[0],
            dst_ref=got.at[of_s, of_r],
            send_sem=send_sem.at[step],
            recv_sem=recv_sem.at[step],
            device_id=(of_r, of_s),
            device_id_type=MESH,
        )

    @pl.loop(1, total)
    def _(step):
        push(step).start()

    @pl.loop(1, total)
    def _(step):
        push(step).wait_send()
        come(step).wait_recv()

    keep.wait()


def swap(mine, reps, shards):
    return pl.pallas_call(
        functools.partial(swap_kernel, reps, shards),
        in_specs=[pl.BlockSpec(memory_space=pltpu.VMEM)],
        out_specs=pl.BlockSpec(memory_space=pltpu.VMEM),
        out_shape=jax.ShapeDtypeStruct((shards, reps) + mine.shape[1:], f32),
        scratch_shapes=[
            pltpu.SemaphoreType.DMA((reps * shards,)),
            pltpu.SemaphoreType.DMA((reps * shards,)),
            pltpu.SemaphoreType.DMA,
        ],
        compiler_params=pltpu.CompilerParams(has_side_effects=True),
        name="swap",
    )(mine)


def regroup(tiles, topk):
    lane = lax.broadcasted_iota(jnp.int32, tiles[0].shape, 1) // topk
    each = LANES // topk
    out = []
    for y in range(each):
        mixed = tiles[y]
        for j in range(each):
            if j != y:
                moved = pltpu.roll(tiles[j], (j - y) % each * topk, axis=1)
                mixed = jnp.where(lane == j, moved, mixed)
        out.append(mixed)
    return out


def scatter(nx, topk, tiles):
    each = LANES // topk
    rows = down(GROUP)
    fields = [[] for _ in range(each)]
    for q in range(0, len(tiles), each):
        for y, tile in enumerate(regroup(tiles[q : q + each], topk)):
            a = jnp.floor(tile * (1.0 / GROUP))
            high, low = split(tile)
            fields[y].append((a, tile - a * GROUP, high.astype(f32), low.astype(f32)))
    grid = []
    for x in range(nx):
        across = []
        for y in range(each):
            ones, values = [], []
            for a, b, high, low in fields[y]:
                at_a = rows == a[nx + x : nx + x + 1]
                at_b = rows == b[nx + x : nx + x + 1]
                plain, scaled = (at_a, at_b) if y % 2 == 0 else (at_b, at_a)
                ones.append(jnp.where(plain, 1.0, 0.0).astype(bf16))
                values.append(jnp.concatenate([
                    jnp.where(scaled, high[x : x + 1], 0.0).astype(bf16),
                    jnp.where(scaled, low[x : x + 1], 0.0).astype(bf16),
                ], axis=0))
            ones, values = jnp.concatenate(ones, axis=1), jnp.concatenate(values, axis=1)
            if y % 2 == 0:
                both = dot_t(ones, values)
                across.append((both + pltpu.roll(both, GROUP, axis=1))[:, :GROUP])
            else:
                both = dot_t(values, ones)
                across.append(both[:GROUP] + both[GROUP:])
        grid.append(jnp.concatenate(across, axis=1))
    return jnp.concatenate(grid, axis=0)


def sum_kernel(nx, topk, reps, _, data, weight, li, ri, smooth_out, weight_out, sums):
    g, last = pl.program_id(0), pl.num_programs(0) - 1

    def gather():
        sums[lax.rem(g, 2)] = scatter(nx, topk, [data[0, r, 0] for r in range(reps)])

    def finish():
        smooth = jnp.tanh(right(left(li[...], sums[lax.rem(g + 1, 2)]), ri[...]))
        smooth_out[...] = smooth.astype(bf16)
        weight_out[...] = (weight[...].astype(f32) - step_rate * smooth).astype(bf16)

    @pl.when(g == 0)
    def _():
        gather()

    @pl.when((g > 0) & (g < last))
    def _():
        finish()
        gather()

    @pl.when(g == last)
    def _():
        finish()


def sum_part(shard, data, weight, topk, interpret=False):
    rows, width = weight.shape
    nx = rows // GROUP
    reps = data.shape[1]
    steps = width // WIDE
    column = pl.BlockSpec((rows, WIDE), lambda g, s: (0, jnp.maximum(g - 1, 0)))
    whole = pl.BlockSpec((2 * PAIR, 2 * PAIR), lambda g, s: (0, 0))
    return pl.pallas_call(
        functools.partial(sum_kernel, nx, topk, reps),
        grid_spec=pltpu.PrefetchScalarGridSpec(
            num_scalar_prefetch=1,
            grid=(steps + 1,),
            in_specs=[
                pl.BlockSpec(
                    (1, reps, 1, 2 * nx, LANES), lambda g, s: (s[0], 0, jnp.minimum(g, steps - 1), 0, 0)
                ),
                column, whole, whole,
            ],
            out_specs=[column, column],
            scratch_shapes=[pltpu.VMEM((2, rows, WIDE), f32)],
        ),
        out_shape=[jax.ShapeDtypeStruct((rows, width), bf16)] * 2,
        interpret=interpret,
        name="sum_part",
    )(shard, data, weight, left_basis(basis().T), right_basis(basis()))


def per_device(reps, shards, weight, momentum, grad, positions):
    rows, width = weight.shape
    _, nx, ny, topk = positions.shape
    half = width // 2
    steps = width // WIDE
    r, s = lax.axis_index("replica"), lax.axis_index("shard")
    core = lax.rem(r, 2)

    mine_w = lax.dynamic_slice(weight, (0, core * half), (rows, half))
    weights = [mine_w] + [
        lax.ppermute(mine_w, "shard", [(i, (i + d) % shards) for i in range(shards)])
        for d in range(1, shards)
    ]

    pos = positions[0].astype(f32).reshape(nx, steps, LANES).transpose(1, 0, 2)
    kept, sent = own_part(momentum, grad, pos, topk)
    got = swap(sent.reshape(2, steps // 2, 2 * nx, LANES), reps, shards)

    pairs = [(i, i ^ 1) for i in range(reps)]
    flip = lambda x: lax.ppermute(x, "replica", pairs)
    order = lambda a, b: [jnp.where(core == 0, a, b), jnp.where(core == 0, b, a)]
    pieces, direction = [], None
    for d in range(shards):
        of = lax.rem(s - d + shards, shards)
        smooth, updated = sum_part(of.reshape(1).astype(jnp.int32), got, weights[d], topk)
        if d == 0:
            direction = jnp.concatenate(order(smooth, flip(smooth)), axis=1)
        pieces.append((updated, flip(updated)))

    columns = []
    for t in range(shards):
        d = lax.rem(s - t + shards, shards)
        a, b = pieces[0]
        for e in range(1, shards):
            a = jnp.where(d == e, pieces[e][0], a)
            b = jnp.where(d == e, pieces[e][1], b)
        columns += order(a, b)
    return (kept, direction, jnp.concatenate(columns, axis=1))


def solution(mesh):
    reps, shards = mesh.shape["replica"], mesh.shape["shard"]
    in_specs = (
        P(None, "shard"),
        P("replica", None, "shard"),
        P("replica", None, "shard"),
        P("replica", None, "shard", None),
    )
    out_specs = (P("replica", None, "shard"), P(None, "shard"), P())
    return jax.shard_map(
        functools.partial(per_device, reps, shards),
        mesh=mesh, in_specs=in_specs, out_specs=out_specs, check_vma=False,
    )
```

```python
import functools
import math

import jax
import jax.numpy as jnp
import numpy as np
from jax import lax
from jax.experimental import pallas as pl
from jax.experimental.pallas import tpu as pltpu
from jax.sharding import PartitionSpec as P

GROUP = 64
LANES = 128
WIDE = 256
PAIR = 128
CHUNKS = 2

beta_decay = 0.9
step_rate = 0.02

f32, bf16 = jnp.float32, jnp.bfloat16
MESH = pl.DeviceIdType.MESH


def basis():
    k = np.arange(GROUP, dtype=np.float64)[:, None]
    i = np.arange(GROUP, dtype=np.float64)[None, :]
    scale = np.where(k == 0, math.sqrt(1.0 / GROUP), math.sqrt(2.0 / GROUP))
    return scale * np.cos(math.pi * (2.0 * i + 1.0) * k / (2.0 * GROUP))


def halves(c):
    full = np.kron(np.eye(PAIR // GROUP), c).astype(np.float32)
    high = full.astype(bf16)
    low = (full - high.astype(np.float32)).astype(bf16)
    return high, low


def left_basis(c):
    high, low = halves(c)
    return np.block([[high, high], [low, low]])


def right_basis(c):
    high, low = halves(c)
    return np.block([[high, low], [high, low]])


def split(x):
    high = x.astype(bf16)
    return high, (x - high.astype(f32)).astype(bf16)


def dot(a, b):
    return jnp.dot(a, b, preferred_element_type=f32)


def dot_t(a, b):
    return lax.dot_general(a, b, (((1,), (1,)), ((), ())), preferred_element_type=f32)


def left(m, x):
    high, low = split(x)
    parts = []
    for at in range(0, x.shape[0], PAIR):
        both = dot(m, jnp.concatenate([high[at : at + PAIR], low[at : at + PAIR]], axis=0))
        parts.append(both[:PAIR] + both[PAIR:])
    return jnp.concatenate(parts, axis=0)


def right(x, m):
    high, low = split(x)
    rows = x.shape[0]
    ats = range(0, x.shape[1], PAIR)
    both = dot(jnp.concatenate([
        jnp.concatenate([high[:, at : at + PAIR], low[:, at : at + PAIR]], axis=1) for at in ats
    ], axis=0), m)
    both = both[:, :PAIR] + both[:, PAIR:]
    return jnp.concatenate([both[i * rows : (i + 1) * rows] for i in range(len(ats))], axis=1)


def down(rows):
    return lax.broadcasted_iota(jnp.int32, (rows, LANES), 0).astype(f32)


def lane_offset(topk):
    lane = lax.broadcasted_iota(jnp.int32, (1, LANES), 1)
    return (lane // topk * GROUP).astype(f32)


def place(pos, topk):
    a = jnp.floor(pos * (1.0 / GROUP))
    return a, pos - a * GROUP + lane_offset(topk)


def own_kernel(nx, topk, reps, shards, mom, grad, pos, places, lf, rt, li, ri, kept, vals, spots, mine, *sems):
    g, steps = pl.program_id(0), pl.num_programs(0)
    lf, rt, li, ri = lf[...], rt[...], li[...], ri[...]
    tiles = mine.shape[1]
    chunk = tiles // CHUNKS
    period = 2 * chunk
    r, s = lax.axis_index("replica"), lax.axis_index("shard")
    me = r * shards + s
    total = reps * shards
    place_send, place_recv, place_own, send_sem, recv_sem, own_sem = sems

    def peer(step):
        to = lax.rem(me + step, total)
        return to // shards, lax.rem(to, shards)

    def place_copy(step):
        to_r, to_s = peer(step)
        return pltpu.make_async_remote_copy(
            src_ref=places.at[lax.rem(to_r, 2)], dst_ref=spots.at[s, r],
            send_sem=place_send.at[step], recv_sem=place_recv.at[step],
            device_id=(to_r, to_s), device_id_type=MESH,
        )

    def value_copy(step, half, c):
        to_r, to_s = peer(step)
        part = pl.ds(c * chunk, chunk)
        return pltpu.make_async_remote_copy(
            src_ref=mine.at[half, part], dst_ref=vals.at[s, r, part],
            send_sem=send_sem.at[c, step], recv_sem=recv_sem.at[c, step],
            device_id=(to_r, to_s), device_id_type=MESH,
        )

    def place_keep():
        return pltpu.make_async_copy(places.at[lax.rem(r, 2)], spots.at[s, r], place_own)

    def value_keep(half, c):
        part = pl.ds(c * chunk, chunk)
        return pltpu.make_async_copy(mine.at[half, part], vals.at[s, r, part], own_sem.at[c])

    @pl.when(g == 0)
    def _():
        place_keep().start()

        @pl.loop(1, total)
        def _(step):
            place_copy(step).start()

    moved = beta_decay * mom[0] + grad[0].astype(f32)
    coeff = right(left(lf, moved), rt)
    at = pos[0]
    a, b = place(at, topk)
    rows, cols = down(GROUP), down(WIDE)
    picked, own = [], []
    for x in range(nx):
        part = coeff[x * GROUP : (x + 1) * GROUP]
        at_row = rows == a[x : x + 1]
        hot_a = jnp.where(at_row, 1.0, 0.0).astype(bf16)
        hot_b = jnp.where(cols == b[x : x + 1], 1.0, 0.0).astype(bf16)
        own.append(part * dot_t(hot_a, hot_b))
        high, low = split(part)
        found = dot(jnp.concatenate([high, low], axis=0), hot_b)
        found = found[:GROUP] + found[GROUP:]
        picked.append(jnp.sum(jnp.where(at_row, found, 0.0), axis=0, keepdims=True))
    kept[0] = moved - right(left(li, jnp.concatenate(own, axis=0)), ri)
    picked = jnp.concatenate(picked, axis=0)
    half_of, tile_of = g // (2 * tiles), lax.rem(g // 2, tiles)
    mine[half_of, tile_of, pl.ds(pl.multiple_of(lax.rem(g, 2) * nx, nx), nx)] = picked

    for half in range(2):
        for c in range(CHUNKS):
            @pl.when(g == half * 2 * tiles + (c + 1) * period - 1)
            def _(half=half, c=c):
                @pl.loop(1, total)
                def _(step):
                    @pl.when(lax.rem(peer(step)[0], 2) == half)
                    def _():
                        value_copy(step, half, c).start()

                @pl.when(lax.rem(r, 2) == half)
                def _():
                    value_keep(half, c).start()

    @pl.when(g == steps - 1)
    def _():
        place_keep().wait()
        for c in range(CHUNKS):
            value_keep(0, c).wait()

        @pl.loop(1, total)
        def _(step):
            of = lax.rem(me - step + total, total)
            of_r, of_s = of // shards, lax.rem(of, shards)
            copy = place_copy(step)
            copy.wait_send()
            pltpu.make_async_remote_copy(
                src_ref=places.at[0], dst_ref=spots.at[of_s, of_r],
                send_sem=place_send.at[step], recv_sem=place_recv.at[step],
                device_id=(of_r, of_s), device_id_type=MESH,
            ).wait_recv()
            for c in range(CHUNKS):
                part = pl.ds(c * chunk, chunk)
                value_copy(step, 0, c).wait_send()
                pltpu.make_async_remote_copy(
                    src_ref=mine.at[0, part], dst_ref=vals.at[of_s, of_r, part],
                    send_sem=send_sem.at[c, step], recv_sem=recv_sem.at[c, step],
                    device_id=(of_r, of_s), device_id_type=MESH,
                ).wait_recv()


def own_part(mom, grad, pos, places, reps, shards, topk):
    _, rows, width = mom.shape
    nx = rows // GROUP
    steps = width // WIDE
    tiles = steps // 4
    total = reps * shards
    whole = pl.BlockSpec((2 * PAIR, 2 * PAIR), lambda g: (0, 0))
    dma = pltpu.SemaphoreType.DMA
    return pl.pallas_call(
        functools.partial(own_kernel, nx, topk, reps, shards),
        grid=(steps,),
        in_specs=[
            pl.BlockSpec((1, rows, WIDE), lambda g: (0, 0, g)),
            pl.BlockSpec((1, rows, WIDE), lambda g: (0, 0, g)),
            pl.BlockSpec((1, nx, LANES), lambda g: (g, 0, 0)),
            pl.BlockSpec(memory_space=pl.ANY),
            whole, whole, whole, whole,
        ],
        out_specs=[
            pl.BlockSpec((1, rows, WIDE), lambda g: (0, 0, g)),
            pl.BlockSpec(memory_space=pl.ANY),
            pl.BlockSpec(memory_space=pl.ANY),
        ],
        out_shape=[
            jax.ShapeDtypeStruct((1, rows, width), f32),
            jax.ShapeDtypeStruct((shards, reps, tiles, 2 * nx, LANES), f32),
            jax.ShapeDtypeStruct((shards, reps) + places.shape[1:], jnp.int16),
        ],
        scratch_shapes=[
            pltpu.VMEM((2, tiles, 2 * nx, LANES), f32),
            dma((total,)), dma((total,)), dma,
            dma((CHUNKS, total)), dma((CHUNKS, total)), dma((CHUNKS,)),
        ],
        compiler_params=pltpu.CompilerParams(has_side_effects=True),
        name="own_part",
    )(
        mom, grad, pos, places,
        left_basis(basis()), right_basis(basis().T),
        left_basis(basis().T), right_basis(basis()),
    )


def regroup(tiles, topk):
    lane = lax.broadcasted_iota(jnp.int32, tiles[0].shape, 1) // topk
    each = LANES // topk
    out = []
    for y in range(each):
        mixed = tiles[y]
        for j in range(each):
            if j != y:
                moved = pltpu.roll(tiles[j], (j - y) % each * topk, axis=1)
                mixed = jnp.where(lane == j, moved, mixed)
        out.append(mixed)
    return out


def scatter(nx, topk, values, spots):
    each = LANES // topk
    rows = down(GROUP)
    fields = [[] for _ in range(each)]
    for q in range(0, len(values), each):
        mixed = zip(regroup(values[q : q + each], topk), regroup(spots[q : q + each], topk))
        for y, (value, spot) in enumerate(mixed):
            a = jnp.floor(spot * (1.0 / GROUP))
            high, low = split(value)
            fields[y].append((a, spot - a * GROUP, high.astype(f32), low.astype(f32)))
    grid = []
    for x in range(nx):
        across = []
        for y in range(each):
            ones, scaled = [], []
            for a, b, high, low in fields[y]:
                at_a = rows == a[x : x + 1]
                at_b = rows == b[x : x + 1]
                plain, chosen = (at_a, at_b) if y % 2 == 0 else (at_b, at_a)
                ones.append(jnp.where(plain, 1.0, 0.0).astype(bf16))
                scaled.append(jnp.concatenate([
                    jnp.where(chosen, high[x : x + 1], 0.0).astype(bf16),
                    jnp.where(chosen, low[x : x + 1], 0.0).astype(bf16),
                ], axis=0))
            ones, scaled = jnp.concatenate(ones, axis=1), jnp.concatenate(scaled, axis=1)
            if y % 2 == 0:
                both = dot_t(ones, scaled)
                across.append((both + pltpu.roll(both, GROUP, axis=1))[:, :GROUP])
            else:
                both = dot_t(scaled, ones)
                across.append(both[:GROUP] + both[GROUP:])
        grid.append(jnp.concatenate(across, axis=1))
    return jnp.concatenate(grid, axis=0)


def sum_kernel(nx, topk, reps, _, vals, spots, weight, li, ri, smooth_out, weight_out, sums, at):
    g, last = pl.program_id(0), pl.num_programs(0) - 1

    def gather():
        rows = pl.ds(pl.multiple_of(lax.rem(g, 2) * nx, nx), nx)
        tile = g // 2
        sums[lax.rem(g, 2)] = scatter(
            nx, topk, [vals[0, r, 0, rows] for r in range(reps)], [at[r, tile, rows] for r in range(reps)]
        )

    def finish():
        smooth = jnp.tanh(right(left(li[...], sums[lax.rem(g + 1, 2)]), ri[...]))
        smooth_out[...] = smooth.astype(bf16)
        weight_out[...] = (weight[...].astype(f32) - step_rate * smooth).astype(bf16)

    @pl.when(g == 0)
    def _():
        for r in range(reps):
            at[r] = spots[0, r].astype(jnp.int32).astype(f32).reshape(at.shape[1:])
        gather()

    @pl.when((g > 0) & (g < last))
    def _():
        finish()
        gather()

    @pl.when(g == last)
    def _():
        finish()


def sum_part(shard, vals, spots, weight, topk):
    rows, width = weight.shape
    nx = rows // GROUP
    reps, tiles = vals.shape[1:3]
    steps = width // WIDE
    column = pl.BlockSpec((rows, WIDE), lambda g, s: (0, jnp.maximum(g - 1, 0)))
    whole = pl.BlockSpec((2 * PAIR, 2 * PAIR), lambda g, s: (0, 0))
    return pl.pallas_call(
        functools.partial(sum_kernel, nx, topk, reps),
        grid_spec=pltpu.PrefetchScalarGridSpec(
            num_scalar_prefetch=1,
            grid=(steps + 1,),
            in_specs=[
                pl.BlockSpec(
                    (1, reps, 1, 2 * nx, LANES),
                    lambda g, s: (s[0], 0, jnp.minimum(g, steps - 1) // 2, 0, 0),
                ),
                pl.BlockSpec((1,) + spots.shape[1:], lambda g, s: (s[0], 0, 0, 0)),
                column, whole, whole,
            ],
            out_specs=[column, column],
            scratch_shapes=[
                pltpu.VMEM((2, rows, WIDE), f32), pltpu.VMEM((reps, tiles, 2 * nx, LANES), f32),
            ],
        ),
        out_shape=[jax.ShapeDtypeStruct((rows, width), bf16)] * 2,
        name="sum_part",
    )(shard, vals, spots, weight, left_basis(basis().T), right_basis(basis()))


def per_device(reps, shards, weight, momentum, grad, positions):
    rows, width = weight.shape
    _, nx, ny, topk = positions.shape
    half = width // 2
    steps = width // WIDE
    r, s = lax.axis_index("replica"), lax.axis_index("shard")
    core = lax.rem(r, 2)

    mine_w = lax.dynamic_slice(weight, (0, core * half), (rows, half))
    weights = [mine_w] + [
        lax.ppermute(mine_w, "shard", [(i, (i + d) % shards) for i in range(shards)])
        for d in range(1, shards)
    ]

    pos = positions[0].reshape(nx, steps, LANES).transpose(1, 0, 2)
    places = pos.astype(jnp.int16).reshape(2, steps // 2 * nx, LANES)
    kept, vals, spots = own_part(momentum, grad, pos.astype(f32), places, reps, shards, topk)

    pairs = [(i, i ^ 1) for i in range(reps)]
    flip = lambda x: lax.ppermute(x, "replica", pairs)
    order = lambda a, b: [jnp.where(core == 0, a, b), jnp.where(core == 0, b, a)]
    pieces, direction = [], None
    for d in range(shards):
        of = lax.rem(s - d + shards, shards)
        smooth, updated = sum_part(of.reshape(1).astype(jnp.int32), vals, spots, weights[d], topk)
        if d == 0:
            direction = jnp.concatenate(order(smooth, flip(smooth)), axis=1)
        pieces.append((updated, flip(updated)))

    columns = []
    for t in range(shards):
        d = lax.rem(s - t + shards, shards)
        a, b = pieces[0]
        for e in range(1, shards):
            a = jnp.where(d == e, pieces[e][0], a)
            b = jnp.where(d == e, pieces[e][1], b)
        columns += order(a, b)
    return (kept, direction, jnp.concatenate(columns, axis=1))


def solution(mesh):
    reps, shards = mesh.shape["replica"], mesh.shape["shard"]
    in_specs = (
        P(None, "shard"),
        P("replica", None, "shard"),
        P("replica", None, "shard"),
        P("replica", None, "shard", None),
    )
    out_specs = (P("replica", None, "shard"), P(None, "shard"), P())
    return jax.shard_map(
        functools.partial(per_device, reps, shards),
        mesh=mesh, in_specs=in_specs, out_specs=out_specs, check_vma=False,
    )
```

```python
import functools
import math

import jax
import jax.numpy as jnp
import numpy as np
from jax import lax
from jax.experimental import pallas as pl
from jax.experimental.pallas import tpu as pltpu
from jax.sharding import PartitionSpec as P

GROUP = 64
LANES = 128
WIDE = 256
PAIR = 128
CHUNKS = 2

beta_decay = 0.9
step_rate = 0.02

f32, bf16 = jnp.float32, jnp.bfloat16
MESH = pl.DeviceIdType.MESH


def basis():
    k = np.arange(GROUP, dtype=np.float64)[:, None]
    i = np.arange(GROUP, dtype=np.float64)[None, :]
    scale = np.where(k == 0, math.sqrt(1.0 / GROUP), math.sqrt(2.0 / GROUP))
    return scale * np.cos(math.pi * (2.0 * i + 1.0) * k / (2.0 * GROUP))


def halves(c):
    full = np.kron(np.eye(PAIR // GROUP), c).astype(np.float32)
    high = full.astype(bf16)
    low = (full - high.astype(np.float32)).astype(bf16)
    return high, low


def left_basis(c):
    high, low = halves(c)
    return np.block([[high, high], [low, low]])


def right_basis(c):
    high, low = halves(c)
    return np.block([[high, low], [high, low]])


def split(x):
    high = x.astype(bf16)
    return high, (x - high.astype(f32)).astype(bf16)


def dot(a, b):
    return jnp.dot(a, b, preferred_element_type=f32)


def dot_t(a, b):
    return lax.dot_general(a, b, (((1,), (1,)), ((), ())), preferred_element_type=f32)


def left(m, x):
    high, low = split(x)
    parts = []
    for at in range(0, x.shape[0], PAIR):
        both = dot(m, jnp.concatenate([high[at : at + PAIR], low[at : at + PAIR]], axis=0))
        parts.append(both[:PAIR] + both[PAIR:])
    return jnp.concatenate(parts, axis=0)


def right(x, m):
    high, low = split(x)
    rows = x.shape[0]
    ats = range(0, x.shape[1], PAIR)
    both = dot(jnp.concatenate([
        jnp.concatenate([high[:, at : at + PAIR], low[:, at : at + PAIR]], axis=1) for at in ats
    ], axis=0), m)
    both = both[:, :PAIR] + both[:, PAIR:]
    return jnp.concatenate([both[i * rows : (i + 1) * rows] for i in range(len(ats))], axis=1)


def down(rows):
    return lax.broadcasted_iota(jnp.int32, (rows, LANES), 0).astype(f32)


def lane_offset(topk):
    lane = lax.broadcasted_iota(jnp.int32, (1, LANES), 1)
    return (lane // topk * GROUP).astype(f32)


def place(pos, topk):
    a = jnp.floor(pos * (1.0 / GROUP))
    return a, pos - a * GROUP + lane_offset(topk)


def own_kernel(nx, topk, reps, shards, mom, grad, pos, lf, rt, li, ri, kept, vals, spots, mine, at_all, places, *sems):
    g, steps = pl.program_id(0), pl.num_programs(0)
    lf, rt, li, ri = lf[...], rt[...], li[...], ri[...]
    tiles = mine.shape[1]
    chunks = min(CHUNKS, tiles)
    chunk = tiles // chunks
    period = 2 * chunk
    r, s = lax.axis_index("replica"), lax.axis_index("shard")
    me = r * shards + s
    total = reps * shards
    place_send, place_recv, place_own, send_sem, recv_sem, own_sem = sems

    def peer(step):
        to = lax.rem(me + step, total)
        return to // shards, lax.rem(to, shards)

    def place_copy(step):
        to_r, to_s = peer(step)
        return pltpu.make_async_remote_copy(
            src_ref=places.at[lax.rem(to_r, 2)], dst_ref=spots.at[s, r],
            send_sem=place_send.at[step], recv_sem=place_recv.at[step],
            device_id=(to_r, to_s), device_id_type=MESH,
        )

    def value_copy(step, half, c):
        to_r, to_s = peer(step)
        part = pl.ds(c * chunk, chunk)
        return pltpu.make_async_remote_copy(
            src_ref=mine.at[half, part], dst_ref=vals.at[s, r, part],
            send_sem=send_sem.at[c, step], recv_sem=recv_sem.at[c, step],
            device_id=(to_r, to_s), device_id_type=MESH,
        )

    def place_keep():
        return pltpu.make_async_copy(places.at[lax.rem(r, 2)], spots.at[s, r], place_own)

    def value_keep(half, c):
        part = pl.ds(c * chunk, chunk)
        return pltpu.make_async_copy(mine.at[half, part], vals.at[s, r, part], own_sem.at[c])

    @pl.when(g == 0)
    def _():
        for x in range(nx):
            at_all[pl.ds(x, pos.shape[1], stride=nx)] = pos[x].astype(f32)
        each = places.shape[1]
        for half in range(2):
            places[half] = at_all[half * each : (half + 1) * each].astype(jnp.int32).astype(jnp.int16)

    moved = beta_decay * mom[0] + grad[0].astype(f32)
    coeff = right(left(lf, moved), rt)
    at = at_all[pl.ds(pl.multiple_of(g * nx, nx), nx)]
    a, b = place(at, topk)
    rows, cols = down(GROUP), down(WIDE)
    picked, own = [], []
    for x in range(nx):
        part = coeff[x * GROUP : (x + 1) * GROUP]
        at_row = rows == a[x : x + 1]
        hot_a = jnp.where(at_row, 1.0, 0.0).astype(bf16)
        hot_b = jnp.where(cols == b[x : x + 1], 1.0, 0.0).astype(bf16)
        own.append(part * dot_t(hot_a, hot_b))
        high, low = split(part)
        found = dot(jnp.concatenate([high, low], axis=0), hot_b)
        found = found[:GROUP] + found[GROUP:]
        picked.append(jnp.sum(jnp.where(at_row, found, 0.0), axis=0, keepdims=True))
    picked = jnp.concatenate(picked, axis=0)
    half_of, tile_of = g // (2 * tiles), lax.rem(g // 2, tiles)
    mine[half_of, tile_of, pl.ds(pl.multiple_of(lax.rem(g, 2) * nx, nx), nx)] = picked

    kept[0] = moved - right(left(li, jnp.concatenate(own, axis=0)), ri)

    @pl.when(g == 0)
    def _():
        place_keep().start()

        @pl.loop(1, total)
        def _(step):
            place_copy(step).start()

    for half in range(2):
        for c in range(chunks):
            @pl.when(g == half * 2 * tiles + (c + 1) * period - 1)
            def _(half=half, c=c):
                @pl.loop(1, total)
                def _(step):
                    @pl.when(lax.rem(peer(step)[0], 2) == half)
                    def _():
                        value_copy(step, half, c).start()

                @pl.when(lax.rem(r, 2) == half)
                def _():
                    value_keep(half, c).start()

    @pl.when(g == steps - 1)
    def _():
        place_keep().wait()
        for c in range(chunks):
            value_keep(0, c).wait()

        @pl.loop(1, total)
        def _(step):
            of = lax.rem(me - step + total, total)
            of_r, of_s = of // shards, lax.rem(of, shards)
            copy = place_copy(step)
            copy.wait_send()
            pltpu.make_async_remote_copy(
                src_ref=places.at[0], dst_ref=spots.at[of_s, of_r],
                send_sem=place_send.at[step], recv_sem=place_recv.at[step],
                device_id=(of_r, of_s), device_id_type=MESH,
            ).wait_recv()
            for c in range(chunks):
                part = pl.ds(c * chunk, chunk)
                value_copy(step, 0, c).wait_send()
                pltpu.make_async_remote_copy(
                    src_ref=mine.at[0, part], dst_ref=vals.at[of_s, of_r, part],
                    send_sem=send_sem.at[c, step], recv_sem=recv_sem.at[c, step],
                    device_id=(of_r, of_s), device_id_type=MESH,
                ).wait_recv()


def own_part(mom, grad, pos, reps, shards, topk):
    _, rows, width = mom.shape
    nx = rows // GROUP
    steps = width // WIDE
    tiles = steps // 4
    chunks = min(CHUNKS, tiles)
    total = reps * shards
    whole = pl.BlockSpec((2 * PAIR, 2 * PAIR), lambda g: (0, 0))
    dma = pltpu.SemaphoreType.DMA
    return pl.pallas_call(
        functools.partial(own_kernel, nx, topk, reps, shards),
        grid=(steps,),
        in_specs=[
            pl.BlockSpec((1, rows, WIDE), lambda g: (0, 0, g)),
            pl.BlockSpec((1, rows, WIDE), lambda g: (0, 0, g)),
            pl.BlockSpec(pos.shape, lambda g: (0, 0, 0)),
            whole, whole, whole, whole,
        ],
        out_specs=[
            pl.BlockSpec((1, rows, WIDE), lambda g: (0, 0, g)),
            pl.BlockSpec(memory_space=pl.ANY),
            pl.BlockSpec(memory_space=pl.ANY),
        ],
        out_shape=[
            jax.ShapeDtypeStruct((1, rows, width), f32),
            jax.ShapeDtypeStruct((shards, reps, tiles, 2 * nx, LANES), f32),
            jax.ShapeDtypeStruct((shards, reps, steps // 2 * nx, LANES), jnp.int16),
        ],
        scratch_shapes=[
            pltpu.VMEM((2, tiles, 2 * nx, LANES), f32),
            pltpu.VMEM((steps * nx, LANES), f32),
            pltpu.VMEM((2, steps // 2 * nx, LANES), jnp.int16),
            dma((total,)), dma((total,)), dma,
            dma((chunks, total)), dma((chunks, total)), dma((chunks,)),
        ],
        compiler_params=pltpu.CompilerParams(has_side_effects=True),
        name="own_part",
    )(
        mom, grad, pos,
        left_basis(basis()), right_basis(basis().T),
        left_basis(basis().T), right_basis(basis()),
    )


def regroup(tiles, topk):
    lane = lax.broadcasted_iota(jnp.int32, tiles[0].shape, 1) // topk
    each = LANES // topk
    out = []
    for y in range(each):
        mixed = tiles[y]
        for j in range(each):
            if j != y:
                moved = pltpu.roll(tiles[j], (j - y) % each * topk, axis=1)
                mixed = jnp.where(lane == j, moved, mixed)
        out.append(mixed)
    return out


def scatter(nx, topk, values, spots):
    each = LANES // topk
    rows = down(GROUP)
    fields = [[] for _ in range(each)]
    for q in range(0, len(values), each):
        mixed = zip(regroup(values[q : q + each], topk), regroup(spots[q : q + each], topk))
        for y, (value, spot) in enumerate(mixed):
            a = jnp.floor(spot * (1.0 / GROUP))
            high, low = split(value)
            fields[y].append((a, spot - a * GROUP, high.astype(f32), low.astype(f32)))
    grid = []
    for x in range(nx):
        across = []
        for y in range(each):
            ones, scaled = [], []
            for a, b, high, low in fields[y]:
                at_a = rows == a[x : x + 1]
                at_b = rows == b[x : x + 1]
                plain, chosen = (at_a, at_b) if y % 2 == 0 else (at_b, at_a)
                ones.append(jnp.where(plain, 1.0, 0.0).astype(bf16))
                scaled.append(jnp.concatenate([
                    jnp.where(chosen, high[x : x + 1], 0.0).astype(bf16),
                    jnp.where(chosen, low[x : x + 1], 0.0).astype(bf16),
                ], axis=0))
            ones, scaled = jnp.concatenate(ones, axis=1), jnp.concatenate(scaled, axis=1)
            if y % 2 == 0:
                both = dot_t(ones, scaled)
                across.append((both + pltpu.roll(both, GROUP, axis=1))[:, :GROUP])
            else:
                both = dot_t(scaled, ones)
                across.append(both[:GROUP] + both[GROUP:])
        grid.append(jnp.concatenate(across, axis=1))
    return jnp.concatenate(grid, axis=0)


def sum_kernel(nx, topk, reps, first, carries, cuts, held, s, vals, spots, *refs):
    refs = list(refs)
    pieces = [refs.pop(0) for _ in cuts]
    kept_in = refs.pop(0) if carries else None
    li, ri = refs.pop(0), refs.pop(0)
    refs = refs[held:]
    updated_out, weight_out = refs.pop(0), refs.pop(0)
    smooth_out, direction_out = (refs.pop(0), refs.pop(0)) if first else (None, None)
    kept_out = refs.pop(0) if carries else None
    sums, at = refs
    g, last = pl.program_id(0), pl.num_programs(0) - 1

    def gather():
        rows = pl.ds(pl.multiple_of(lax.rem(g, 2) * nx, nx), nx)
        tile = s[1 + g] // 2
        sums[lax.rem(g, 2)] = scatter(
            nx, topk, [vals[0, r, 0, rows] for r in range(reps)], [at[r, tile, rows] for r in range(reps)]
        )

    def finish():
        smooth = jnp.tanh(right(left(li[...], sums[lax.rem(g + 1, 2)]), ri[...]))
        weight = pieces[0][...]
        for cut, piece in zip(cuts[1:], pieces[1:]):
            weight = jnp.where(g > cut, piece[...], weight)
        updated = (weight.astype(f32) - step_rate * smooth).astype(bf16)
        updated_out[...] = updated
        weight_out[...] = updated
        if first:
            direction = smooth.astype(bf16)
            smooth_out[...] = direction
            direction_out[...] = direction
        if carries:
            kept_out[...] = kept_in[...]

    @pl.when(g == 0)
    def _():
        for r in range(reps):
            at[r] = spots[0, r].astype(jnp.int32).astype(f32).reshape(at.shape[1:])
        gather()

    @pl.when((g > 0) & (g < last))
    def _():
        finish()
        gather()

    @pl.when(g == last)
    def _():
        finish()


def sum_part(d, scalars, vals, spots, pieces, kept, held, topk):
    rows, reps, tiles = pieces[0][0].shape[0], vals.shape[1], vals.shape[2]
    nx = rows // GROUP
    shards = vals.shape[0]
    steps = 2 * tiles
    width = 2 * steps * WIDE
    first, carries = d == 0, d < 2
    now = lambda g: jnp.minimum(g, steps - 1)
    before = lambda g: jnp.maximum(g - 1, 0)
    cuts, specs = [], []
    for array, offset, count in pieces:
        cut = sum(n for _, _, n in pieces[: len(cuts)])
        cuts.append(cut)
        if offset:
            specs.append(pl.BlockSpec((rows, WIDE), lambda g, s: (0, s[1 + steps + before(g)])))
        else:
            specs.append(pl.BlockSpec(
                (rows, WIDE), lambda g, s, cut=cut, n=count: (0, jnp.clip(before(g) - cut, 0, n - 1))
            ))
    whole = pl.BlockSpec((2 * PAIR, 2 * PAIR), lambda g, s: (0, 0))
    column = lambda at: pl.BlockSpec((rows, WIDE), lambda g, s: (0, s[1 + at * steps + before(g)]))
    kept_spec = pl.BlockSpec((1, rows, WIDE), lambda g, s: (0, 0, d * steps + before(g)))
    in_specs = [
        pl.BlockSpec((1, reps, 1, 2 * nx, LANES), lambda g, s: (s[0], 0, s[1 + now(g)] // 2, 0, 0)),
        pl.BlockSpec((1,) + spots.shape[1:], lambda g, s: (s[0], 0, 0, 0)),
    ] + specs + ([kept_spec] if carries else []) + [whole, whole]
    in_specs += [pl.BlockSpec(memory_space=pl.ANY)] * len(held)
    half = jax.ShapeDtypeStruct((rows, width // 2), bf16)
    out_specs, out_shape = [column(0), column(2)], [half, jax.ShapeDtypeStruct((rows, shards * width), bf16)]
    if first:
        out_specs += [column(0), column(1)]
        out_shape += [half, jax.ShapeDtypeStruct((rows, width), bf16)]
    if carries:
        out_specs.append(kept_spec)
        out_shape.append(jax.ShapeDtypeStruct((1, rows, width), f32))
    at = 1 + len(in_specs) - len(held)
    targets = [1, 2][: len(held)]
    return pl.pallas_call(
        functools.partial(sum_kernel, nx, topk, reps, first, carries, cuts, len(held)),
        grid_spec=pltpu.PrefetchScalarGridSpec(
            num_scalar_prefetch=1,
            grid=(steps + 1,),
            in_specs=in_specs,
            out_specs=out_specs,
            scratch_shapes=[
                pltpu.VMEM((2, rows, WIDE), f32), pltpu.VMEM((reps, tiles, 2 * nx, LANES), f32),
            ],
        ),
        out_shape=out_shape,
        input_output_aliases={at + i: t for i, t in enumerate(targets)},
        cost_estimate=pl.CostEstimate(flops=steps * 2 * 10**9, bytes_accessed=8 * 2**20, transcendentals=0),
        name="sum_part",
    )(
        scalars, vals, spots, *[array for array, _, _ in pieces], *([kept] if carries else []),
        left_basis(basis().T), right_basis(basis()), *held,
    )


def place_kernel(count, _, *refs):
    for i in range(count):
        refs[2 * count + i][...] = refs[i][...]


def put(blocks, parts, fulls):
    rows, width = parts[0].shape
    wide = math.gcd(width, 1024)
    count, steps = len(parts), width // wide
    def spec(i):
        return pl.BlockSpec((rows, wide), lambda g, s: (0, s[i] * steps + g))
    return pl.pallas_call(
        functools.partial(place_kernel, count),
        grid_spec=pltpu.PrefetchScalarGridSpec(
            num_scalar_prefetch=1,
            grid=(steps,),
            in_specs=[pl.BlockSpec((rows, wide), lambda g, s: (0, g))] * count
            + [pl.BlockSpec(memory_space=pl.ANY)] * count,
            out_specs=[spec(i) for i in range(count)],
        ),
        out_shape=[jax.ShapeDtypeStruct(f.shape, f.dtype) for f in fulls],
        input_output_aliases={1 + count + i: i for i in range(count)},
        cost_estimate=pl.CostEstimate(flops=0, bytes_accessed=4 * count * rows * width, transcendentals=0),
        name="put",
    )(blocks, *parts, *fulls)


def per_device(reps, shards, weight, momentum, grad, positions):
    rows, width = weight.shape
    _, nx, ny, topk = positions.shape
    half = width // 2
    steps = half // WIDE
    r, s = lax.axis_index("replica"), lax.axis_index("shard")
    core = lax.rem(r, 2)
    spread = reps % 8 == 0 and steps % 4 == 0
    side = ((r // 2) + (r // 4)) % 2 if spread else 0 * r

    def ring(x, d):
        return lax.ppermute(x, "shard", [(i, (i + d) % shards) for i in range(shards)])

    def across(x, bit):
        return lax.ppermute(x, "replica", [(i, i ^ bit) for i in range(reps)])

    others = []
    units = np.arange(steps)
    if spread:
        part = half // 2
        mine = lax.dynamic_slice(weight, (0, core * half + side * part), (rows, part))
        for d in range(1, shards):
            near = ring(mine, d)
            others.append((near, across(near[:, : part // 2], 2), across(near[:, part // 2 :], 4)))
        order = (units + side * (steps // 2)) % steps
    else:
        mine = lax.dynamic_slice(weight, (0, core * half), (rows, half))
        others = [(ring(mine, d),) for d in range(1, shards)]
        order = jnp.asarray(units)

    pos = positions[0].reshape(nx, 2 * steps, LANES)
    kept, vals, spots = own_part(momentum, grad, pos, reps, shards, topk)

    def scalars(of, order):
        base = core * steps + order
        return jnp.concatenate([of.reshape(1), order, base, of * 2 * steps + base]).astype(jnp.int32)

    updated, new_weight, smooth, direction, kept_full = sum_part(
        0, scalars(s, jnp.asarray(units)), vals, spots, [(weight, True, steps)], kept, (), topk
    )
    parts = [(s, updated)]
    for d in range(1, shards):
        of = lax.rem(s - d + shards, shards)
        pieces = [(w, False, w.shape[1] // WIDE) for w in others[d - 1]]
        held = (new_weight, kept_full) if d == 1 else (new_weight,)
        out = sum_part(d, scalars(of, order), vals, spots, pieces, kept, held, topk)
        updated, new_weight = out[0], out[1]
        if d == 1:
            kept_full = out[2]
        parts.append((of, updated))

    far = 1 - core
    block = lambda *at: jnp.stack(at).astype(jnp.int32)
    new_weight, direction = put(
        block(s * 2 + far, far), [across(parts[0][1], 1), across(smooth, 1)], [new_weight, direction]
    )
    for of, piece in parts[1:]:
        new_weight, = put(block(of * 2 + far), [across(piece, 1)], [new_weight])
    return (kept_full, direction, new_weight)


def solution(mesh):
    reps, shards = mesh.shape["replica"], mesh.shape["shard"]
    in_specs = (
        P(None, "shard"),
        P("replica", None, "shard"),
        P("replica", None, "shard"),
        P("replica", None, "shard", None),
    )
    out_specs = (P("replica", None, "shard"), P(None, "shard"), P())
    return jax.shard_map(
        functools.partial(per_device, reps, shards),
        mesh=mesh, in_specs=in_specs, out_specs=out_specs, check_vma=False,
    )
```

```python
import functools
import math

import jax
import jax.numpy as jnp
import numpy as np
from jax import lax
from jax.experimental import pallas as pl
from jax.experimental.pallas import tpu as pltpu
from jax.sharding import PartitionSpec as P

GROUP = 64
LANES = 128
WIDE = 256
PAIR = 128

beta_decay = 0.9
step_rate = 0.02

f32, bf16 = jnp.float32, jnp.bfloat16
MESH = pl.DeviceIdType.MESH


def basis():
    k = np.arange(GROUP, dtype=np.float64)[:, None]
    i = np.arange(GROUP, dtype=np.float64)[None, :]
    scale = np.where(k == 0, math.sqrt(1.0 / GROUP), math.sqrt(2.0 / GROUP))
    return scale * np.cos(math.pi * (2.0 * i + 1.0) * k / (2.0 * GROUP))


def halves(c):
    full = np.kron(np.eye(PAIR // GROUP), c).astype(np.float32)
    high = full.astype(bf16)
    low = (full - high.astype(np.float32)).astype(bf16)
    return high, low


def left_basis(c):
    high, low = halves(c)
    return np.block([[high, high], [low, low]])


def right_basis(c):
    high, low = halves(c)
    return np.block([[high, low], [high, low]])


def split(x):
    high = x.astype(bf16)
    return high, (x - high.astype(f32)).astype(bf16)


def dot(a, b):
    return jnp.dot(a, b, preferred_element_type=f32)


def dot_t(a, b):
    return lax.dot_general(a, b, (((1,), (1,)), ((), ())), preferred_element_type=f32)


def left(m, x):
    high, low = split(x)
    parts = []
    for at in range(0, x.shape[0], PAIR):
        both = dot(m, jnp.concatenate([high[at : at + PAIR], low[at : at + PAIR]], axis=0))
        parts.append(both[:PAIR] + both[PAIR:])
    return jnp.concatenate(parts, axis=0)


def right(x, m):
    high, low = split(x)
    rows = x.shape[0]
    ats = range(0, x.shape[1], PAIR)
    both = dot(jnp.concatenate([
        jnp.concatenate([high[:, at : at + PAIR], low[:, at : at + PAIR]], axis=1) for at in ats
    ], axis=0), m)
    both = both[:, :PAIR] + both[:, PAIR:]
    return jnp.concatenate([both[i * rows : (i + 1) * rows] for i in range(len(ats))], axis=1)


def down(rows):
    return lax.broadcasted_iota(jnp.int32, (rows, LANES), 0).astype(f32)


def lane_offset(topk):
    lane = lax.broadcasted_iota(jnp.int32, (1, LANES), 1)
    return (lane // topk * GROUP).astype(f32)


def place(pos, topk):
    a = jnp.floor(pos * (1.0 / GROUP))
    return a, pos - a * GROUP + lane_offset(topk)


def cut_points(tiles):
    return sorted({0, tiles // 2, tiles - 1, tiles} - {-1})


def own_kernel(nx, topk, reps, shards, mom, grad, pos, lf, rt, li, ri, kept, vals, spots, mine, at_all, places, *sems):
    g, steps = pl.program_id(0), pl.num_programs(0)
    lf, rt, li, ri = lf[...], rt[...], li[...], ri[...]
    tiles = mine.shape[1]
    cuts = cut_points(tiles)
    chunks = len(cuts) - 1
    r, s = lax.axis_index("replica"), lax.axis_index("shard")
    me = r * shards + s
    total = reps * shards
    place_send, place_recv, place_own, send_sem, recv_sem, own_sem = sems

    def peer(step):
        to = lax.rem(me + step, total)
        return to // shards, lax.rem(to, shards)

    def place_copy(step):
        to_r, to_s = peer(step)
        return pltpu.make_async_remote_copy(
            src_ref=places.at[lax.rem(to_r, 2)], dst_ref=spots.at[s, r],
            send_sem=place_send.at[step], recv_sem=place_recv.at[step],
            device_id=(to_r, to_s), device_id_type=MESH,
        )

    def value_copy(step, half, c):
        to_r, to_s = peer(step)
        part = pl.ds(cuts[c], cuts[c + 1] - cuts[c])
        return pltpu.make_async_remote_copy(
            src_ref=mine.at[half, part], dst_ref=vals.at[s, r, part],
            send_sem=send_sem.at[c, step], recv_sem=recv_sem.at[c, step],
            device_id=(to_r, to_s), device_id_type=MESH,
        )

    def place_keep():
        return pltpu.make_async_copy(places.at[lax.rem(r, 2)], spots.at[s, r], place_own)

    def value_keep(half, c):
        part = pl.ds(cuts[c], cuts[c + 1] - cuts[c])
        return pltpu.make_async_copy(mine.at[half, part], vals.at[s, r, part], own_sem.at[c])

    @pl.when(g == 0)
    def _():
        barrier = pltpu.get_barrier_semaphore()

        @pl.loop(1, total)
        def _(step):
            pl.semaphore_signal(barrier, inc=1, device_id=peer(step), device_id_type=MESH)

        for x in range(nx):
            at_all[pl.ds(x, pos.shape[1], stride=nx)] = pos[x].astype(f32)
        each = places.shape[1]
        for half in range(2):
            places[half] = at_all[half * each : (half + 1) * each].astype(jnp.int32).astype(jnp.int16)

    moved = beta_decay * mom[0] + grad[0].astype(f32)
    coeff = right(left(lf, moved), rt)
    at = at_all[pl.ds(pl.multiple_of(g * nx, nx), nx)]
    a, b = place(at, topk)
    rows, cols = down(GROUP), down(WIDE)
    picked, own = [], []
    for x in range(nx):
        part = coeff[x * GROUP : (x + 1) * GROUP]
        at_row = rows == a[x : x + 1]
        hot_a = jnp.where(at_row, 1.0, 0.0).astype(bf16)
        hot_b = jnp.where(cols == b[x : x + 1], 1.0, 0.0).astype(bf16)
        own.append(part * dot_t(hot_a, hot_b))
        high, low = split(part)
        found = dot(jnp.concatenate([high, low], axis=0), hot_b)
        found = found[:GROUP] + found[GROUP:]
        picked.append(jnp.sum(jnp.where(at_row, found, 0.0), axis=0, keepdims=True))
    picked = jnp.concatenate(picked, axis=0)
    half_of, tile_of = g // (2 * tiles), lax.rem(g // 2, tiles)
    mine[half_of, tile_of, pl.ds(pl.multiple_of(lax.rem(g, 2) * nx, nx), nx)] = picked

    kept[0] = moved - right(left(li, jnp.concatenate(own, axis=0)), ri)

    @pl.when(g == 0)
    def _():
        pl.semaphore_wait(pltpu.get_barrier_semaphore(), total - 1)
        place_keep().start()

        @pl.loop(1, total)
        def _(step):
            place_copy(step).start()

    for half in range(2):
        for c in range(chunks):
            @pl.when(g == 2 * (half * tiles + cuts[c + 1]) - 1)
            def _(half=half, c=c):
                @pl.loop(1, total)
                def _(step):
                    @pl.when(lax.rem(peer(step)[0], 2) == half)
                    def _():
                        value_copy(step, half, c).start()

                @pl.when(lax.rem(r, 2) == half)
                def _():
                    value_keep(half, c).start()

    @pl.when(g == steps - 1)
    def _():
        place_keep().wait()
        for c in range(chunks):
            value_keep(0, c).wait()

        @pl.loop(1, total)
        def _(step):
            of = lax.rem(me - step + total, total)
            of_r, of_s = of // shards, lax.rem(of, shards)
            copy = place_copy(step)
            copy.wait_send()
            pltpu.make_async_remote_copy(
                src_ref=places.at[0], dst_ref=spots.at[of_s, of_r],
                send_sem=place_send.at[step], recv_sem=place_recv.at[step],
                device_id=(of_r, of_s), device_id_type=MESH,
            ).wait_recv()
            for c in range(chunks):
                part = pl.ds(cuts[c], cuts[c + 1] - cuts[c])
                value_copy(step, 0, c).wait_send()
                pltpu.make_async_remote_copy(
                    src_ref=mine.at[0, part], dst_ref=vals.at[of_s, of_r, part],
                    send_sem=send_sem.at[c, step], recv_sem=recv_sem.at[c, step],
                    device_id=(of_r, of_s), device_id_type=MESH,
                ).wait_recv()


def own_part(mom, grad, pos, reps, shards, topk):
    _, rows, width = mom.shape
    nx = rows // GROUP
    steps = width // WIDE
    tiles = steps // 4
    chunks = len(cut_points(tiles)) - 1
    total = reps * shards
    whole = pl.BlockSpec((2 * PAIR, 2 * PAIR), lambda g: (0, 0))
    dma = pltpu.SemaphoreType.DMA
    return pl.pallas_call(
        functools.partial(own_kernel, nx, topk, reps, shards),
        grid=(steps,),
        in_specs=[
            pl.BlockSpec((1, rows, WIDE), lambda g: (0, 0, g)),
            pl.BlockSpec((1, rows, WIDE), lambda g: (0, 0, g)),
            pl.BlockSpec(pos.shape, lambda g: (0, 0, 0)),
            whole, whole, whole, whole,
        ],
        out_specs=[
            pl.BlockSpec((1, rows, WIDE), lambda g: (0, 0, g)),
            pl.BlockSpec(memory_space=pl.ANY),
            pl.BlockSpec(memory_space=pl.ANY),
        ],
        out_shape=[
            jax.ShapeDtypeStruct((1, rows, width), f32),
            jax.ShapeDtypeStruct((shards, reps, tiles, 2 * nx, LANES), f32),
            jax.ShapeDtypeStruct((shards, reps, steps // 2 * nx, LANES), jnp.int16),
        ],
        scratch_shapes=[
            pltpu.VMEM((2, tiles, 2 * nx, LANES), f32),
            pltpu.VMEM((steps * nx, LANES), f32),
            pltpu.VMEM((2, steps // 2 * nx, LANES), jnp.int16),
            dma((total,)), dma((total,)), dma,
            dma((chunks, total)), dma((chunks, total)), dma((chunks,)),
        ],
        compiler_params=pltpu.CompilerParams(has_side_effects=True, collective_id=0),
        name="own_part",
    )(
        mom, grad, pos,
        left_basis(basis()), right_basis(basis().T),
        left_basis(basis().T), right_basis(basis()),
    )


def regroup(tiles, topk):
    lane = lax.broadcasted_iota(jnp.int32, tiles[0].shape, 1) // topk
    each = LANES // topk
    out = []
    for y in range(each):
        mixed = tiles[y]
        for j in range(each):
            if j != y:
                moved = pltpu.roll(tiles[j], (j - y) % each * topk, axis=1)
                mixed = jnp.where(lane == j, moved, mixed)
        out.append(mixed)
    return out


def scatter(nx, topk, values, spots):
    each = LANES // topk
    rows = down(GROUP)
    fields = [[] for _ in range(each)]
    for q in range(0, len(values), each):
        mixed = zip(regroup(values[q : q + each], topk), regroup(spots[q : q + each], topk))
        for y, (value, spot) in enumerate(mixed):
            a = jnp.floor(spot * (1.0 / GROUP))
            high, low = split(value)
            fields[y].append((a, spot - a * GROUP, high.astype(f32), low.astype(f32)))
    grid = []
    for x in range(nx):
        across = []
        for y in range(each):
            ones, scaled = [], []
            for a, b, high, low in fields[y]:
                at_a = rows == a[x : x + 1]
                at_b = rows == b[x : x + 1]
                plain, chosen = (at_a, at_b) if y % 2 == 0 else (at_b, at_a)
                ones.append(jnp.where(plain, 1.0, 0.0).astype(bf16))
                scaled.append(jnp.concatenate([
                    jnp.where(chosen, high[x : x + 1], 0.0).astype(bf16),
                    jnp.where(chosen, low[x : x + 1], 0.0).astype(bf16),
                ], axis=0))
            ones, scaled = jnp.concatenate(ones, axis=1), jnp.concatenate(scaled, axis=1)
            if y % 2 == 0:
                both = dot_t(ones, scaled)
                across.append((both + pltpu.roll(both, GROUP, axis=1))[:, :GROUP])
            else:
                both = dot_t(scaled, ones)
                across.append(both[:GROUP] + both[GROUP:])
        grid.append(jnp.concatenate(across, axis=1))
    return jnp.concatenate(grid, axis=0)


def sum_kernel(nx, topk, reps, first, carries, base, cuts, held, s, vals, spots, *refs):
    refs = list(refs)
    pieces = [refs.pop(0) for _ in cuts]
    kept_in = refs.pop(0) if carries else None
    li, ri = refs.pop(0), refs.pop(0)
    refs = refs[held:]
    updated_out, weight_out = refs.pop(0), refs.pop(0)
    smooth_out, direction_out = (refs.pop(0), refs.pop(0)) if first else (None, None)
    kept_out = refs.pop(0) if carries else None
    sums, at, hold, in_sem, out_sem = refs
    g, last = pl.program_id(0), pl.num_programs(0) - 1

    def gather():
        rows = pl.ds(pl.multiple_of(lax.rem(g, 2) * nx, nx), nx)
        tile = s[1 + g] // 2
        sums[lax.rem(g, 2)] = scatter(
            nx, topk, [vals[0, r, 0, rows] for r in range(reps)], [at[r, tile, rows] for r in range(reps)]
        )

    def finish():
        smooth = jnp.tanh(right(left(li[...], sums[lax.rem(g + 1, 2)]), ri[...]))
        weight = pieces[0][...]
        for cut, piece in zip(cuts[1:], pieces[1:]):
            weight = jnp.where(g > cut, piece[...], weight)
        updated = (weight.astype(f32) - step_rate * smooth).astype(bf16)
        updated_out[...] = updated
        weight_out[...] = updated
        if first:
            direction = smooth.astype(bf16)
            smooth_out[...] = direction
            direction_out[...] = direction

    def column(step):
        return pl.ds(pl.multiple_of((base + step) * WIDE, WIDE), WIDE)

    def bring(step):
        slot = lax.rem(step, 2)
        return pltpu.make_async_copy(kept_in.at[0, :, column(step)], hold.at[slot], in_sem.at[slot])

    def drop(step):
        slot = lax.rem(step, 2)
        return pltpu.make_async_copy(hold.at[slot], kept_out.at[0, :, column(step)], out_sem.at[slot])

    if carries:
        @pl.when((g > 1) & (g < last))
        def _():
            drop(g - 2).wait()

        @pl.when(g < last)
        def _():
            bring(g).start()

        @pl.when(g > 0)
        def _():
            bring(g - 1).wait()
            drop(g - 1).start()

    @pl.when(g == 0)
    def _():
        for r in range(reps):
            at[r] = spots[0, r].astype(jnp.int32).astype(f32).reshape(at.shape[1:])
        gather()

    @pl.when((g > 0) & (g < last))
    def _():
        finish()
        gather()

    @pl.when(g == last)
    def _():
        finish()
        if carries:
            drop(g - 2).wait()
            drop(g - 1).wait()


def sum_part(d, scalars, vals, spots, pieces, kept, held, topk):
    rows, reps, tiles = pieces[0][0].shape[0], vals.shape[1], vals.shape[2]
    nx = rows // GROUP
    shards = vals.shape[0]
    steps = 2 * tiles
    width = 2 * steps * WIDE
    first, carries = d == 0, d < 2
    now = lambda g: jnp.minimum(g, steps - 1)
    before = lambda g: jnp.maximum(g - 1, 0)
    cuts, specs = [], []
    for array, offset, count in pieces:
        cut = sum(n for _, _, n in pieces[: len(cuts)])
        cuts.append(cut)
        if offset:
            specs.append(pl.BlockSpec((rows, WIDE), lambda g, s: (0, s[1 + steps + before(g)])))
        else:
            specs.append(pl.BlockSpec(
                (rows, WIDE), lambda g, s, cut=cut, n=count: (0, jnp.clip(before(g) - cut, 0, n - 1))
            ))
    whole = pl.BlockSpec((2 * PAIR, 2 * PAIR), lambda g, s: (0, 0))
    column = lambda at: pl.BlockSpec((rows, WIDE), lambda g, s: (0, s[1 + at * steps + before(g)]))
    kept_spec = pl.BlockSpec(memory_space=pl.ANY)
    in_specs = [
        pl.BlockSpec((1, reps, 1, 2 * nx, LANES), lambda g, s: (s[0], 0, s[1 + now(g)] // 2, 0, 0)),
        pl.BlockSpec((1,) + spots.shape[1:], lambda g, s: (s[0], 0, 0, 0)),
    ] + specs + ([kept_spec] if carries else []) + [whole, whole]
    in_specs += [pl.BlockSpec(memory_space=pl.ANY)] * len(held)
    half = jax.ShapeDtypeStruct((rows, width // 2), bf16)
    out_specs, out_shape = [column(0), column(2)], [half, jax.ShapeDtypeStruct((rows, shards * width), bf16)]
    if first:
        out_specs += [column(0), column(1)]
        out_shape += [half, jax.ShapeDtypeStruct((rows, width), bf16)]
    if carries:
        out_specs.append(kept_spec)
        out_shape.append(jax.ShapeDtypeStruct((1, rows, width), f32))
    at = 1 + len(in_specs) - len(held)
    targets = [1, 2][: len(held)]
    return pl.pallas_call(
        functools.partial(sum_kernel, nx, topk, reps, first, carries, d * steps, cuts, len(held)),
        grid_spec=pltpu.PrefetchScalarGridSpec(
            num_scalar_prefetch=1,
            grid=(steps + 1,),
            in_specs=in_specs,
            out_specs=out_specs,
            scratch_shapes=[
                pltpu.VMEM((2, rows, WIDE), f32), pltpu.VMEM((reps, tiles, 2 * nx, LANES), f32),
                pltpu.VMEM((2, rows, WIDE), f32), pltpu.SemaphoreType.DMA((2,)), pltpu.SemaphoreType.DMA((2,)),
            ],
        ),
        out_shape=out_shape,
        input_output_aliases={at + i: t for i, t in enumerate(targets)},
        cost_estimate=pl.CostEstimate(flops=steps * 2 * 10**9, bytes_accessed=8 * 2**20, transcendentals=0),
        name="sum_part",
    )(
        scalars, vals, spots, *[array for array, _, _ in pieces], *([kept] if carries else []),
        left_basis(basis().T), right_basis(basis()), *held,
    )


def place_kernel(count, shards, blocks, *refs):
    r, s = lax.axis_index("replica"), lax.axis_index("shard")
    far = 1 - lax.rem(r, 2)
    sems = refs[-1]
    copies = []
    for i in range(count):
        part, full = refs[i], refs[2 * count + i]
        width = part.shape[1]
        block = far if blocks[i] is None else 2 * lax.rem(s + blocks[i], shards) + far
        at = pl.ds(pl.multiple_of(block * width, width), width)
        copies.append(pltpu.make_async_copy(part, full.at[:, at], sems.at[i]))
    for copy in copies:
        copy.start()
    for copy in copies:
        copy.wait()


def put(shards, blocks, parts, fulls):
    count = len(parts)
    return pl.pallas_call(
        functools.partial(place_kernel, count, shards, blocks),
        in_specs=[pl.BlockSpec(memory_space=pl.ANY)] * (2 * count),
        out_specs=[pl.BlockSpec(memory_space=pl.ANY)] * count,
        out_shape=[jax.ShapeDtypeStruct(f.shape, f.dtype) for f in fulls],
        scratch_shapes=[pltpu.SemaphoreType.DMA((count,))],
        input_output_aliases={count + i: i for i in range(count)},
        cost_estimate=pl.CostEstimate(flops=0, bytes_accessed=2 * count * parts[0].size, transcendentals=0),
        compiler_params=pltpu.CompilerParams(vmem_limit_bytes=2**20),
        name="put",
    )(*parts, *fulls)


def per_device(reps, shards, weight, momentum, grad, positions):
    rows, width = weight.shape
    _, nx, ny, topk = positions.shape
    half = width // 2
    steps = half // WIDE
    r, s = lax.axis_index("replica"), lax.axis_index("shard")
    core = lax.rem(r, 2)
    def ring(x, d):
        return lax.ppermute(x, "shard", [(i, (i + d) % shards) for i in range(shards)])

    def across(x, bit):
        return lax.ppermute(x, "replica", [(i, i ^ bit) for i in range(reps)])

    mine = lax.dynamic_slice(weight, (0, core * half), (rows, half))
    others = [ring(mine, d) for d in range(1, shards)]

    pos = positions[0].reshape(nx, 2 * steps, LANES)
    kept, vals, spots = own_part(momentum, grad, pos, reps, shards, topk)

    units = np.arange(steps)

    def scalars(of):
        base = core * steps + units
        return jnp.concatenate([of.reshape(1), jnp.asarray(units), base, of * 2 * steps + base]).astype(jnp.int32)

    updated, new_weight, smooth, direction, kept_full = sum_part(
        0, scalars(s), vals, spots, [(weight, True, steps)], kept, (), topk
    )
    parts = [updated]
    for d in range(1, shards):
        of = lax.rem(s - d + shards, shards)
        held = (new_weight, kept_full) if d == 1 else (new_weight,)
        out = sum_part(d, scalars(of), vals, spots, [(others[d - 1], False, steps)], kept, held, topk)
        updated, new_weight = out[0], out[1]
        if d == 1:
            kept_full = out[2]
        parts.append(updated)

    new_weight, direction = put(
        shards, [0, None], [across(parts[0], 1), across(smooth, 1)], [new_weight, direction]
    )
    for d in range(1, shards):
        new_weight, = put(shards, [shards - d], [across(parts[d], 1)], [new_weight])
    return (kept_full, direction, new_weight)


def solution(mesh):
    reps, shards = mesh.shape["replica"], mesh.shape["shard"]
    in_specs = (
        P(None, "shard"),
        P("replica", None, "shard"),
        P("replica", None, "shard"),
        P("replica", None, "shard", None),
    )
    out_specs = (P("replica", None, "shard"), P(None, "shard"), P())
    return jax.shard_map(
        functools.partial(per_device, reps, shards),
        mesh=mesh, in_specs=in_specs, out_specs=out_specs, check_vma=False,
    )
```

```python
import functools
import math

import jax
import jax.numpy as jnp
import numpy as np
from jax import lax
from jax.experimental import pallas as pl
from jax.experimental.pallas import tpu as pltpu
from jax.sharding import PartitionSpec as P

GROUP = 64
LANES = 128
WIDE = 256
PAIR = 128

beta_decay = 0.9
step_rate = 0.02

f32, bf16 = jnp.float32, jnp.bfloat16
MESH = pl.DeviceIdType.MESH


def basis():
    k = np.arange(GROUP, dtype=np.float64)[:, None]
    i = np.arange(GROUP, dtype=np.float64)[None, :]
    scale = np.where(k == 0, math.sqrt(1.0 / GROUP), math.sqrt(2.0 / GROUP))
    return scale * np.cos(math.pi * (2.0 * i + 1.0) * k / (2.0 * GROUP))


def halves(c):
    full = np.kron(np.eye(PAIR // GROUP), c).astype(np.float32)
    high = full.astype(bf16)
    low = (full - high.astype(np.float32)).astype(bf16)
    return high, low


def left_basis(c):
    high, low = halves(c)
    return np.block([[high, high], [low, low]])


def right_basis(c):
    high, low = halves(c)
    return np.block([[high, low], [high, low]])


def split(x):
    high = x.astype(bf16)
    return high, (x - high.astype(f32)).astype(bf16)


def dot(a, b):
    return jnp.dot(a, b, preferred_element_type=f32)


def dot_t(a, b):
    return lax.dot_general(a, b, (((1,), (1,)), ((), ())), preferred_element_type=f32)


def left(m, x):
    high, low = split(x)
    parts = []
    for at in range(0, x.shape[0], PAIR):
        both = dot(m, jnp.concatenate([high[at : at + PAIR], low[at : at + PAIR]], axis=0))
        parts.append(both[:PAIR] + both[PAIR:])
    return jnp.concatenate(parts, axis=0)


def right(x, m):
    high, low = split(x)
    rows = x.shape[0]
    ats = range(0, x.shape[1], PAIR)
    both = dot(jnp.concatenate([
        jnp.concatenate([high[:, at : at + PAIR], low[:, at : at + PAIR]], axis=1) for at in ats
    ], axis=0), m)
    both = both[:, :PAIR] + both[:, PAIR:]
    return jnp.concatenate([both[i * rows : (i + 1) * rows] for i in range(len(ats))], axis=1)


def down(rows):
    return lax.broadcasted_iota(jnp.int32, (rows, LANES), 0).astype(f32)


def lane_offset(topk):
    lane = lax.broadcasted_iota(jnp.int32, (1, LANES), 1)
    return (lane // topk * GROUP).astype(f32)


def place(pos, topk):
    a = jnp.floor(pos * (1.0 / GROUP))
    return a, pos - a * GROUP + lane_offset(topk)


def cut_points(half, tiles):
    return sorted({0, tiles - 1, tiles}) if half else [0, tiles]


def own_kernel(
    nx, topk, reps, shards, mom, grad, pos, lf, rt, li, ri, kept, vals, spots,
    mine, at_all, places, old, turned, place_send, place_recv, send_sem, recv_sem,
):
    g, last = pl.program_id(0), pl.num_programs(0) - 1
    tiles = mine.shape[1]
    r, s = lax.axis_index("replica"), lax.axis_index("shard")
    me = s * reps + r
    total = reps * shards

    def peer(step):
        to = lax.rem(me + step, total)
        return lax.rem(to, reps), to // reps

    def place_copy(step):
        to_r, to_s = peer(step)
        return pltpu.make_async_remote_copy(
            src_ref=places.at[lax.rem(to_r, 2)], dst_ref=spots.at[me],
            send_sem=place_send, recv_sem=place_recv, device_id=(to_r, to_s), device_id_type=MESH,
        )

    def value_copy(step, half, part):
        to = lax.rem(me // 2 + step, total // 2)
        to_s, to_r = to // (reps // 2), 2 * lax.rem(to, reps // 2) + half
        return pltpu.make_async_remote_copy(
            src_ref=mine.at[half, part], dst_ref=vals.at[me, part],
            send_sem=send_sem, recv_sem=recv_sem, device_id=(to_r, to_s), device_id_type=MESH,
        )

    def forward():
        moved = beta_decay * mom[0] + grad[0].astype(f32)
        slot = lax.rem(g, 2)
        old[slot] = moved
        turned[slot] = right(left(lf[...], moved), rt[...])

    def backward():
        u, slot = g - 1, lax.rem(g + 1, 2)
        a, b = place(at_all[pl.ds(pl.multiple_of(u * nx, nx), nx)], topk)
        rows, cols = down(GROUP), down(WIDE)
        picked, own = [], []
        for x in range(nx):
            part = turned[slot, x * GROUP : (x + 1) * GROUP]
            at_row = rows == a[x : x + 1]
            hot_a = jnp.where(at_row, 1.0, 0.0).astype(bf16)
            hot_b = jnp.where(cols == b[x : x + 1], 1.0, 0.0).astype(bf16)
            own.append(part * dot_t(hot_a, hot_b))
            high, low = split(part)
            found = dot(jnp.concatenate([high, low], axis=0), hot_b)
            found = found[:GROUP] + found[GROUP:]
            picked.append(jnp.sum(jnp.where(at_row, found, 0.0), axis=0, keepdims=True))
        rows_at = pl.ds(pl.multiple_of(lax.rem(u, 2) * nx, nx), nx)
        mine[u // (2 * tiles), lax.rem(u // 2, tiles), rows_at] = jnp.concatenate(picked, axis=0)
        kept[0] = old[slot] - right(left(li[...], jnp.concatenate(own, axis=0)), ri[...])

    @pl.when(g == 0)
    def _():
        barrier = pltpu.get_barrier_semaphore()

        @pl.loop(1, total)
        def _(step):
            pl.semaphore_signal(barrier, inc=1, device_id=peer(step), device_id_type=MESH)

        for x in range(nx):
            at_all[pl.ds(x, pos.shape[1], stride=nx)] = pos[x].astype(f32)
        each = places.shape[1]
        for half in range(2):
            places[half] = at_all[half * each : (half + 1) * each].astype(jnp.int32).astype(jnp.int16)
        forward()
        pl.semaphore_wait(barrier, total - 1)
        pltpu.make_async_copy(places.at[lax.rem(r, 2)], spots.at[me], place_recv).start()

        @pl.loop(1, total)
        def _(step):
            place_copy(step).start()

    @pl.when((g > 0) & (g < last))
    def _():
        backward()
        forward()

    @pl.when(g == last)
    def _():
        backward()

    for half in range(2):
        cuts = cut_points(half, tiles)
        for begin, end in zip(cuts[:-1], cuts[1:]):
            @pl.when(g == 2 * (half * tiles + end))
            def _(half=half, part=pl.ds(begin, end - begin)):
                @pl.when(lax.rem(r, 2) == half)
                def _():
                    pltpu.make_async_copy(mine.at[half, part], vals.at[me, part], recv_sem).start()

                @pl.when(lax.rem(r, 2) != half)
                def _():
                    value_copy(0, half, part).start()

                @pl.loop(1, total // 2)
                def _(step):
                    value_copy(step, half, part).start()

    @pl.when(g == last)
    def _():
        most = pl.ds(0, total - 1)
        pltpu.make_async_copy(spots.at[most], spots.at[most], place_send).wait()
        pltpu.make_async_copy(spots, spots, place_recv).wait()
        pltpu.make_async_copy(vals.at[most], vals.at[most], send_sem).wait()
        pltpu.make_async_copy(vals, vals, recv_sem).wait()


def own_part(mom, grad, pos, reps, shards, topk):
    _, rows, width = mom.shape
    nx = rows // GROUP
    steps = width // WIDE
    tiles = steps // 4
    total = reps * shards
    whole = pl.BlockSpec((2 * PAIR, 2 * PAIR), lambda g: (0, 0))
    now = pl.BlockSpec((1, rows, WIDE), lambda g: (0, 0, jnp.minimum(g, steps - 1)))
    dma = pltpu.SemaphoreType.DMA
    return pl.pallas_call(
        functools.partial(own_kernel, nx, topk, reps, shards),
        grid=(steps + 1,),
        in_specs=[
            now, now,
            pl.BlockSpec(pos.shape, lambda g: (0, 0, 0)),
            whole, whole, whole, whole,
        ],
        out_specs=[
            pl.BlockSpec((1, rows, WIDE), lambda g: (0, 0, jnp.maximum(g - 1, 0))),
            pl.BlockSpec(memory_space=pl.ANY),
            pl.BlockSpec(memory_space=pl.ANY),
        ],
        out_shape=[
            jax.ShapeDtypeStruct((1, rows, width), f32),
            jax.ShapeDtypeStruct((total, tiles, 2 * nx, LANES), f32),
            jax.ShapeDtypeStruct((total, steps // 2 * nx, LANES), jnp.int16),
        ],
        scratch_shapes=[
            pltpu.VMEM((2, tiles, 2 * nx, LANES), f32),
            pltpu.VMEM((steps * nx, LANES), f32),
            pltpu.VMEM((2, steps // 2 * nx, LANES), jnp.int16),
            pltpu.VMEM((2, rows, WIDE), f32), pltpu.VMEM((2, rows, WIDE), f32),
            dma, dma, dma, dma,
        ],
        compiler_params=pltpu.CompilerParams(has_side_effects=True, collective_id=0),
        name="own_part",
    )(
        mom, grad, pos,
        left_basis(basis()), right_basis(basis().T),
        left_basis(basis().T), right_basis(basis()),
    )


def regroup(tiles, topk):
    lane = lax.broadcasted_iota(jnp.int32, tiles[0].shape, 1) // topk
    each = LANES // topk
    out = []
    for y in range(each):
        mixed = tiles[y]
        for j in range(each):
            if j != y:
                moved = pltpu.roll(tiles[j], (j - y) % each * topk, axis=1)
                mixed = jnp.where(lane == j, moved, mixed)
        out.append(mixed)
    return out


def scatter(nx, topk, values, spots):
    each = LANES // topk
    rows = down(GROUP)
    fields = [[] for _ in range(each)]
    for q in range(0, len(values), each):
        mixed = zip(regroup(values[q : q + each], topk), regroup(spots[q : q + each], topk))
        for y, (value, spot) in enumerate(mixed):
            a = jnp.floor(spot * (1.0 / GROUP))
            high, low = split(value)
            fields[y].append((a, spot - a * GROUP, high.astype(f32), low.astype(f32)))
    grid = []
    for x in range(nx):
        across = []
        for y in range(each):
            ones, scaled = [], []
            for a, b, high, low in fields[y]:
                at_a = rows == a[x : x + 1]
                at_b = rows == b[x : x + 1]
                plain, chosen = (at_a, at_b) if y % 2 == 0 else (at_b, at_a)
                ones.append(jnp.where(plain, 1.0, 0.0).astype(bf16))
                scaled.append(jnp.concatenate([
                    jnp.where(chosen, high[x : x + 1], 0.0).astype(bf16),
                    jnp.where(chosen, low[x : x + 1], 0.0).astype(bf16),
                ], axis=0))
            ones, scaled = jnp.concatenate(ones, axis=1), jnp.concatenate(scaled, axis=1)
            if y % 2 == 0:
                both = dot_t(ones, scaled)
                across.append((both + pltpu.roll(both, GROUP, axis=1))[:, :GROUP])
            else:
                both = dot_t(scaled, ones)
                across.append(both[:GROUP] + both[GROUP:])
        grid.append(jnp.concatenate(across, axis=1))
    return jnp.concatenate(grid, axis=0)


def sum_kernel(nx, topk, reps, first, carries, base, cuts, held, s, vals, spots, *refs):
    refs = list(refs)
    pieces = [refs.pop(0) for _ in cuts]
    kept_in = refs.pop(0) if carries else None
    li, ri = refs.pop(0), refs.pop(0)
    refs = refs[held:]
    updated_out, weight_out = refs.pop(0), refs.pop(0)
    smooth_out, direction_out = (refs.pop(0), refs.pop(0)) if first else (None, None)
    kept_out = refs.pop(0) if carries else None
    sums, at, hold, in_sem, out_sem = refs
    g, last = pl.program_id(0), pl.num_programs(0) - 1

    def gather():
        rows = pl.ds(pl.multiple_of(lax.rem(g, 2) * nx, nx), nx)
        tile = g // 2
        sums[lax.rem(g, 2)] = scatter(
            nx, topk, [vals[r, 0, rows] for r in range(reps)], [at[r, tile, rows] for r in range(reps)]
        )

    def finish():
        smooth = jnp.tanh(right(left(li[...], sums[lax.rem(g + 1, 2)]), ri[...]))
        weight = pieces[0][...]
        for cut, piece in zip(cuts[1:], pieces[1:]):
            weight = jnp.where(g > cut, piece[...], weight)
        updated = (weight.astype(f32) - step_rate * smooth).astype(bf16)
        updated_out[...] = updated
        weight_out[...] = updated
        if first:
            direction = smooth.astype(bf16)
            smooth_out[...] = direction
            direction_out[...] = direction

    def column(step):
        return pl.ds(pl.multiple_of((base + step) * WIDE, WIDE), WIDE)

    def bring(step):
        slot = lax.rem(step, 2)
        return pltpu.make_async_copy(kept_in.at[0, :, column(step)], hold.at[slot], in_sem.at[slot])

    def drop(step):
        slot = lax.rem(step, 2)
        return pltpu.make_async_copy(hold.at[slot], kept_out.at[0, :, column(step)], out_sem.at[slot])

    if carries:
        @pl.when((g > 1) & (g < last))
        def _():
            drop(g - 2).wait()

        @pl.when(g < last)
        def _():
            bring(g).start()

        @pl.when(g > 0)
        def _():
            bring(g - 1).wait()
            drop(g - 1).start()

    @pl.when(g == 0)
    def _():
        for r in range(reps):
            at[r] = spots[r].astype(jnp.int32).astype(f32).reshape(at.shape[1:])
        gather()

    @pl.when((g > 0) & (g < last))
    def _():
        finish()
        gather()

    @pl.when(g == last)
    def _():
        finish()
        if carries:
            drop(g - 2).wait()
            drop(g - 1).wait()


def sum_part(d, shards, scalars, vals, spots, pieces, kept, held, topk):
    rows, reps, tiles = pieces[0][0].shape[0], vals.shape[0] // shards, vals.shape[1]
    nx = rows // GROUP
    steps = 2 * tiles
    width = 2 * steps * WIDE
    first, carries = d == 0, d < 2
    now = lambda g: jnp.minimum(g, steps - 1)
    before = lambda g: jnp.maximum(g - 1, 0)
    cuts, specs = [], []
    for array, offset, count in pieces:
        cut = sum(n for _, _, n in pieces[: len(cuts)])
        cuts.append(cut)
        if offset:
            specs.append(pl.BlockSpec((rows, WIDE), lambda g, s: (0, s[2] + before(g))))
        else:
            specs.append(pl.BlockSpec(
                (rows, WIDE), lambda g, s, cut=cut, n=count: (0, jnp.clip(before(g) - cut, 0, n - 1))
            ))
    whole = pl.BlockSpec((2 * PAIR, 2 * PAIR), lambda g, s: (0, 0))
    column = lambda at: pl.BlockSpec((rows, WIDE), lambda g, s: (0, s[1 + at] + before(g)))
    kept_spec = pl.BlockSpec(memory_space=pl.ANY)
    in_specs = [
        pl.BlockSpec((reps, 1, 2 * nx, LANES), lambda g, s: (s[0], now(g) // 2, 0, 0)),
        pl.BlockSpec((reps,) + spots.shape[1:], lambda g, s: (s[0], 0, 0)),
    ] + specs + ([kept_spec] if carries else []) + [whole, whole]
    in_specs += [pl.BlockSpec(memory_space=pl.ANY)] * len(held)
    half = jax.ShapeDtypeStruct((rows, width // 2), bf16)
    out_specs, out_shape = [column(0), column(2)], [half, jax.ShapeDtypeStruct((rows, shards * width), bf16)]
    if first:
        out_specs += [column(0), column(1)]
        out_shape += [half, jax.ShapeDtypeStruct((rows, width), bf16)]
    if carries:
        out_specs.append(kept_spec)
        out_shape.append(jax.ShapeDtypeStruct((1, rows, width), f32))
    at = 1 + len(in_specs) - len(held)
    targets = [1, 2][: len(held)]
    return pl.pallas_call(
        functools.partial(sum_kernel, nx, topk, reps, first, carries, d * steps, cuts, len(held)),
        grid_spec=pltpu.PrefetchScalarGridSpec(
            num_scalar_prefetch=1,
            grid=(steps + 1,),
            in_specs=in_specs,
            out_specs=out_specs,
            scratch_shapes=[
                pltpu.VMEM((2, rows, WIDE), f32), pltpu.VMEM((reps, tiles, 2 * nx, LANES), f32),
                pltpu.VMEM((2, rows, WIDE), f32), pltpu.SemaphoreType.DMA((2,)), pltpu.SemaphoreType.DMA((2,)),
            ],
        ),
        out_shape=out_shape,
        input_output_aliases={at + i: t for i, t in enumerate(targets)},
        cost_estimate=pl.CostEstimate(flops=steps * 2 * 10**9, bytes_accessed=8 * 2**20, transcendentals=0),
        name="sum_part",
    )(
        scalars, vals, spots, *[array for array, _, _ in pieces], *([kept] if carries else []),
        left_basis(basis().T), right_basis(basis()), *held,
    )


def place_kernel(count, shards, blocks, *refs):
    r, s = lax.axis_index("replica"), lax.axis_index("shard")
    far = 1 - lax.rem(r, 2)
    sems = refs[-1]
    copies = []
    for i in range(count):
        part, full = refs[i], refs[2 * count + i]
        width = part.shape[1]
        block = far if blocks[i] is None else 2 * lax.rem(s + blocks[i], shards) + far
        at = pl.ds(pl.multiple_of(block * width, width), width)
        copies.append(pltpu.make_async_copy(part, full.at[:, at], sems.at[i]))
    for copy in copies:
        copy.start()
    for copy in copies:
        copy.wait()


def put(shards, blocks, parts, fulls):
    count = len(parts)
    return pl.pallas_call(
        functools.partial(place_kernel, count, shards, blocks),
        in_specs=[pl.BlockSpec(memory_space=pl.ANY)] * (2 * count),
        out_specs=[pl.BlockSpec(memory_space=pl.ANY)] * count,
        out_shape=[jax.ShapeDtypeStruct(f.shape, f.dtype) for f in fulls],
        scratch_shapes=[pltpu.SemaphoreType.DMA((count,))],
        input_output_aliases={count + i: i for i in range(count)},
        cost_estimate=pl.CostEstimate(flops=0, bytes_accessed=2 * count * parts[0].size, transcendentals=0),
        compiler_params=pltpu.CompilerParams(vmem_limit_bytes=2**20),
        name="put",
    )(*parts, *fulls)


def per_device(reps, shards, weight, momentum, grad, positions):
    rows, width = weight.shape
    _, nx, ny, topk = positions.shape
    half = width // 2
    steps = half // WIDE
    r, s = lax.axis_index("replica"), lax.axis_index("shard")
    core = lax.rem(r, 2)
    def ring(x, d):
        return lax.ppermute(x, "shard", [(i, (i + d) % shards) for i in range(shards)])

    def across(x, bit):
        return lax.ppermute(x, "replica", [(i, i ^ bit) for i in range(reps)])

    mine = lax.dynamic_slice(weight, (0, core * half), (rows, half))
    others = [ring(mine, d) for d in range(1, shards)]

    pos = positions[0].reshape(nx, 2 * steps, LANES)
    kept, vals, spots = own_part(momentum, grad, pos, reps, shards, topk)

    def scalars(of):
        return jnp.stack([of, 0 * of, core * steps, (of * 2 + core) * steps]).astype(jnp.int32)

    updated, new_weight, smooth, direction, kept_full = sum_part(
        0, shards, scalars(s), vals, spots, [(weight, True, steps)], kept, (), topk
    )
    parts = [updated]
    for d in range(1, shards):
        of = lax.rem(s - d + shards, shards)
        held = (new_weight, kept_full) if d == 1 else (new_weight,)
        out = sum_part(d, shards, scalars(of), vals, spots, [(others[d - 1], False, steps)], kept, held, topk)
        updated, new_weight = out[0], out[1]
        if d == 1:
            kept_full = out[2]
        parts.append(updated)

    new_weight, direction = put(
        shards, [0, None], [across(parts[0], 1), across(smooth, 1)], [new_weight, direction]
    )
    for d in range(1, shards):
        new_weight, = put(shards, [shards - d], [across(parts[d], 1)], [new_weight])
    return (kept_full, direction, new_weight)


def solution(mesh):
    reps, shards = mesh.shape["replica"], mesh.shape["shard"]
    in_specs = (
        P(None, "shard"),
        P("replica", None, "shard"),
        P("replica", None, "shard"),
        P("replica", None, "shard", None),
    )
    out_specs = (P("replica", None, "shard"), P(None, "shard"), P())
    return jax.shard_map(
        functools.partial(per_device, reps, shards),
        mesh=mesh, in_specs=in_specs, out_specs=out_specs, check_vma=False,
    )
```

```python
import functools
import math

import jax
import jax.numpy as jnp
import numpy as np
from jax import lax
from jax.experimental import pallas as pl
from jax.experimental.pallas import tpu as pltpu
from jax.sharding import PartitionSpec as P

GROUP = 64
LANES = 128
WIDE = 256
PAIR = 128

beta_decay = 0.9
step_rate = 0.02

f32, bf16 = jnp.float32, jnp.bfloat16
MESH = pl.DeviceIdType.MESH


def basis():
    k = np.arange(GROUP, dtype=np.float64)[:, None]
    i = np.arange(GROUP, dtype=np.float64)[None, :]
    scale = np.where(k == 0, math.sqrt(1.0 / GROUP), math.sqrt(2.0 / GROUP))
    return scale * np.cos(math.pi * (2.0 * i + 1.0) * k / (2.0 * GROUP))


def halves(c):
    full = np.kron(np.eye(PAIR // GROUP), c).astype(np.float32)
    high = full.astype(bf16)
    low = (full - high.astype(np.float32)).astype(bf16)
    return high, low


def left_basis(c):
    high, low = halves(c)
    return np.block([[high, high], [low, low]])


def right_basis(c):
    high, low = halves(c)
    return np.block([[high, low], [high, low]])


def split(x):
    high = x.astype(bf16)
    return high, (x - high.astype(f32)).astype(bf16)


def dot(a, b):
    return jnp.dot(a, b, preferred_element_type=f32)


def dot_t(a, b):
    return lax.dot_general(a, b, (((1,), (1,)), ((), ())), preferred_element_type=f32)


def left(m, x):
    high, low = split(x)
    parts = []
    for at in range(0, x.shape[0], PAIR):
        both = dot(m, jnp.concatenate([high[at : at + PAIR], low[at : at + PAIR]], axis=0))
        parts.append(both[:PAIR] + both[PAIR:])
    return jnp.concatenate(parts, axis=0)


def right(x, m):
    high, low = split(x)
    rows = x.shape[0]
    ats = range(0, x.shape[1], PAIR)
    both = dot(jnp.concatenate([
        jnp.concatenate([high[:, at : at + PAIR], low[:, at : at + PAIR]], axis=1) for at in ats
    ], axis=0), m)
    both = both[:, :PAIR] + both[:, PAIR:]
    return jnp.concatenate([both[i * rows : (i + 1) * rows] for i in range(len(ats))], axis=1)


def down(rows):
    return lax.broadcasted_iota(jnp.int32, (rows, LANES), 0).astype(f32)


def lane_offset(topk):
    lane = lax.broadcasted_iota(jnp.int32, (1, LANES), 1)
    return (lane // topk * GROUP).astype(f32)


def place(pos, topk):
    a = jnp.floor(pos * (1.0 / GROUP))
    return a, pos - a * GROUP + lane_offset(topk)


def chunks_of(tiles):
    halves = [sorted({0, tiles // 2, tiles}), sorted({0, tiles // 2, tiles - 1, tiles})]
    pieces = [(h, a, b) for h in range(2) for a, b in zip(halves[h][:-1], halves[h][1:])]
    ready = [2 * (h * tiles + b) for h, _, b in pieces]
    windows = [b - a for a, b in zip(ready[:-1], ready[1:])] + [1]
    return list(zip(pieces, ready, windows))


def own_kernel(
    nx, topk, reps, shards, mom, grad, pos, lf, rt, li, ri, kept, vals, spots,
    mine, at_all, places, old, turned, place_send, place_recv, send_sem, recv_sem,
):
    g, last = pl.program_id(0), pl.num_programs(0) - 1
    tiles = mine.shape[1]
    r, s = lax.axis_index("replica"), lax.axis_index("shard")
    me = s * reps + r
    total = reps * shards

    def peer(step):
        to = lax.rem(me + step, total)
        return lax.rem(to, reps), to // reps

    def place_copy(step):
        to_r, to_s = peer(step)
        return pltpu.make_async_remote_copy(
            src_ref=places.at[lax.rem(to_r, 2)], dst_ref=spots.at[me],
            send_sem=place_send, recv_sem=place_recv, device_id=(to_r, to_s), device_id_type=MESH,
        )

    def value_copy(step, half, part):
        to = lax.rem(me // 2 + step, total // 2)
        to_s, to_r = to // (reps // 2), 2 * lax.rem(to, reps // 2) + half
        return pltpu.make_async_remote_copy(
            src_ref=mine.at[half, part], dst_ref=vals.at[me, part],
            send_sem=send_sem, recv_sem=recv_sem, device_id=(to_r, to_s), device_id_type=MESH,
        )

    def forward():
        moved = beta_decay * mom[0] + grad[0].astype(f32)
        slot = lax.rem(g, 2)
        old[slot] = moved
        turned[slot] = right(left(lf[...], moved), rt[...])

    def backward():
        u, slot = g - 1, lax.rem(g + 1, 2)
        a, b = place(at_all[pl.ds(pl.multiple_of(u * nx, nx), nx)], topk)
        rows, cols = down(GROUP), down(WIDE)
        picked, own = [], []
        for x in range(nx):
            part = turned[slot, x * GROUP : (x + 1) * GROUP]
            at_row = rows == a[x : x + 1]
            hot_a = jnp.where(at_row, 1.0, 0.0).astype(bf16)
            hot_b = jnp.where(cols == b[x : x + 1], 1.0, 0.0).astype(bf16)
            own.append(part * dot_t(hot_a, hot_b))
            high, low = split(part)
            found = dot(jnp.concatenate([high, low], axis=0), hot_b)
            found = found[:GROUP] + found[GROUP:]
            picked.append(jnp.sum(jnp.where(at_row, found, 0.0), axis=0, keepdims=True))
        rows_at = pl.ds(pl.multiple_of(lax.rem(u, 2) * nx, nx), nx)
        mine[u // (2 * tiles), lax.rem(u // 2, tiles), rows_at] = jnp.concatenate(picked, axis=0)
        kept[0] = old[slot] - right(left(li[...], jnp.concatenate(own, axis=0)), ri[...])

    @pl.when(g == 0)
    def _():
        barrier = pltpu.get_barrier_semaphore()

        @pl.loop(1, total)
        def _(step):
            pl.semaphore_signal(barrier, inc=1, device_id=peer(step), device_id_type=MESH)

        for x in range(nx):
            at_all[pl.ds(x, pos.shape[1], stride=nx)] = pos[x].astype(f32)
        each = places.shape[1]
        for half in range(2):
            places[half] = at_all[half * each : (half + 1) * each].astype(jnp.int32).astype(jnp.int16)
        forward()
        pl.semaphore_wait(barrier, total - 1)
        pltpu.make_async_copy(places.at[lax.rem(r, 2)], spots.at[me], place_recv).start()

    @pl.when((g > 0) & (g < last))
    def _():
        backward()
        forward()

    @pl.when(g == last)
    def _():
        backward()

    share = -(-(total - 1) // tiles)

    @pl.when(g < last)
    def _():
        @pl.loop(1 + g * share, jnp.minimum(1 + (g + 1) * share, total))
        def _(step):
            place_copy(step).start()

    for (half, begin, end), ready, window in chunks_of(tiles):
        each = -(-(total // 2) // window)

        @pl.when((g >= ready) & (g < ready + window))
        def _(half=half, part=pl.ds(begin, end - begin), ready=ready, each=each):
            start = (g - ready) * each

            @pl.when((g == ready) & (lax.rem(r, 2) == half))
            def _():
                pltpu.make_async_copy(mine.at[half, part], vals.at[me, part], recv_sem).start()

            @pl.when((g == ready) & (lax.rem(r, 2) != half))
            def _():
                value_copy(0, half, part).start()

            @pl.loop(jnp.maximum(start, 1), jnp.minimum(start + each, total // 2))
            def _(step):
                value_copy(step, half, part).start()

    @pl.when(g == last)
    def _():
        most = pl.ds(0, total - 1)
        pltpu.make_async_copy(spots.at[most], spots.at[most], place_send).wait()
        pltpu.make_async_copy(spots, spots, place_recv).wait()
        pltpu.make_async_copy(vals.at[most], vals.at[most], send_sem).wait()
        pltpu.make_async_copy(vals, vals, recv_sem).wait()


def own_part(mom, grad, pos, reps, shards, topk):
    _, rows, width = mom.shape
    nx = rows // GROUP
    steps = width // WIDE
    tiles = steps // 4
    total = reps * shards
    whole = pl.BlockSpec((2 * PAIR, 2 * PAIR), lambda g: (0, 0))
    now = pl.BlockSpec((1, rows, WIDE), lambda g: (0, 0, jnp.minimum(g, steps - 1)))
    dma = pltpu.SemaphoreType.DMA
    return pl.pallas_call(
        functools.partial(own_kernel, nx, topk, reps, shards),
        grid=(steps + 1,),
        in_specs=[
            now, now,
            pl.BlockSpec(pos.shape, lambda g: (0, 0, 0)),
            whole, whole, whole, whole,
        ],
        out_specs=[
            pl.BlockSpec((1, rows, WIDE), lambda g: (0, 0, jnp.maximum(g - 1, 0))),
            pl.BlockSpec(memory_space=pl.ANY),
            pl.BlockSpec(memory_space=pl.ANY),
        ],
        out_shape=[
            jax.ShapeDtypeStruct((1, rows, width), f32),
            jax.ShapeDtypeStruct((total, tiles, 2 * nx, LANES), f32),
            jax.ShapeDtypeStruct((total, steps // 2 * nx, LANES), jnp.int16),
        ],
        scratch_shapes=[
            pltpu.VMEM((2, tiles, 2 * nx, LANES), f32),
            pltpu.VMEM((steps * nx, LANES), f32),
            pltpu.VMEM((2, steps // 2 * nx, LANES), jnp.int16),
            pltpu.VMEM((2, rows, WIDE), f32), pltpu.VMEM((2, rows, WIDE), f32),
            dma, dma, dma, dma,
        ],
        compiler_params=pltpu.CompilerParams(has_side_effects=True, collective_id=0),
        name="own_part",
    )(
        mom, grad, pos,
        left_basis(basis()), right_basis(basis().T),
        left_basis(basis().T), right_basis(basis()),
    )


def regroup(tiles, topk):
    lane = lax.broadcasted_iota(jnp.int32, tiles[0].shape, 1) // topk
    each = LANES // topk
    out = []
    for y in range(each):
        mixed = tiles[y]
        for j in range(each):
            if j != y:
                moved = pltpu.roll(tiles[j], (j - y) % each * topk, axis=1)
                mixed = jnp.where(lane == j, moved, mixed)
        out.append(mixed)
    return out


def scatter(nx, topk, values, spots):
    each = LANES // topk
    rows = down(GROUP)
    fields = [[] for _ in range(each)]
    for q in range(0, len(values), each):
        mixed = zip(regroup(values[q : q + each], topk), regroup(spots[q : q + each], topk))
        for y, (value, spot) in enumerate(mixed):
            a = jnp.floor(spot * (1.0 / GROUP))
            high, low = split(value)
            fields[y].append((a, spot - a * GROUP, high.astype(f32), low.astype(f32)))
    grid = []
    for x in range(nx):
        across = []
        for y in range(each):
            ones, scaled = [], []
            for a, b, high, low in fields[y]:
                at_a = rows == a[x : x + 1]
                at_b = rows == b[x : x + 1]
                plain, chosen = (at_a, at_b) if y % 2 == 0 else (at_b, at_a)
                ones.append(jnp.where(plain, 1.0, 0.0).astype(bf16))
                scaled.append(jnp.concatenate([
                    jnp.where(chosen, high[x : x + 1], 0.0).astype(bf16),
                    jnp.where(chosen, low[x : x + 1], 0.0).astype(bf16),
                ], axis=0))
            ones, scaled = jnp.concatenate(ones, axis=1), jnp.concatenate(scaled, axis=1)
            if y % 2 == 0:
                both = dot_t(ones, scaled)
                across.append((both + pltpu.roll(both, GROUP, axis=1))[:, :GROUP])
            else:
                both = dot_t(scaled, ones)
                across.append(both[:GROUP] + both[GROUP:])
        grid.append(jnp.concatenate(across, axis=1))
    return jnp.concatenate(grid, axis=0)


def sum_kernel(nx, topk, reps, first, carries, base, cuts, held, of, near, wide, vals, spots, *refs):
    refs = list(refs)
    pieces = [refs.pop(0) for _ in cuts]
    kept_in = refs.pop(0) if carries else None
    li, ri = refs.pop(0), refs.pop(0)
    refs = refs[held:]
    updated_out, weight_out = refs.pop(0), refs.pop(0)
    smooth_out, direction_out = (refs.pop(0), refs.pop(0)) if first else (None, None)
    kept_out = refs.pop(0) if carries else None
    sums, at, hold, in_sem, out_sem = refs
    g, last = pl.program_id(0), pl.num_programs(0) - 1

    def gather():
        rows = pl.ds(pl.multiple_of(lax.rem(g, 2) * nx, nx), nx)
        tile = g // 2
        sums[lax.rem(g, 2)] = scatter(
            nx, topk, [vals[r, 0, rows] for r in range(reps)], [at[r, tile, rows] for r in range(reps)]
        )

    def finish():
        smooth = jnp.tanh(right(left(li[...], sums[lax.rem(g + 1, 2)]), ri[...]))
        weight = pieces[0][...]
        for cut, piece in zip(cuts[1:], pieces[1:]):
            weight = jnp.where(g > cut, piece[...], weight)
        updated = (weight.astype(f32) - step_rate * smooth).astype(bf16)
        updated_out[...] = updated
        weight_out[...] = updated
        if first:
            direction = smooth.astype(bf16)
            smooth_out[...] = direction
            direction_out[...] = direction

    def column(step):
        return pl.ds(pl.multiple_of((base + step) * WIDE, WIDE), WIDE)

    def bring(step):
        slot = lax.rem(step, 2)
        return pltpu.make_async_copy(kept_in.at[0, :, column(step)], hold.at[slot], in_sem.at[slot])

    def drop(step):
        slot = lax.rem(step, 2)
        return pltpu.make_async_copy(hold.at[slot], kept_out.at[0, :, column(step)], out_sem.at[slot])

    if carries:
        @pl.when((g > 1) & (g < last))
        def _():
            drop(g - 2).wait()

        @pl.when(g < last)
        def _():
            bring(g).start()

        @pl.when(g > 0)
        def _():
            bring(g - 1).wait()
            drop(g - 1).start()

    @pl.when(g == 0)
    def _():
        for r in range(reps):
            at[r] = spots[r].astype(jnp.int32).astype(f32).reshape(at.shape[1:])
        gather()

    @pl.when((g > 0) & (g < last))
    def _():
        finish()
        gather()

    @pl.when(g == last)
    def _():
        finish()
        if carries:
            drop(g - 2).wait()
            drop(g - 1).wait()


def sum_part(d, shards, scalars, vals, spots, pieces, kept, held, topk):
    rows, reps, tiles = pieces[0][0].shape[0], vals.shape[0] // shards, vals.shape[1]
    nx = rows // GROUP
    steps = 2 * tiles
    width = 2 * steps * WIDE
    first, carries = d == 0, d < 2
    now = lambda g: jnp.minimum(g, steps - 1)
    before = lambda g: jnp.maximum(g - 1, 0)
    cuts, specs = [], []
    for array, offset, count in pieces:
        cut = sum(n for _, _, n in pieces[: len(cuts)])
        cuts.append(cut)
        if offset:
            specs.append(pl.BlockSpec((rows, WIDE), lambda g, *s: (0, s[1][0] + before(g))))
        else:
            specs.append(pl.BlockSpec(
                (rows, WIDE), lambda g, *s, cut=cut, n=count: (0, jnp.clip(before(g) - cut, 0, n - 1))
            ))
    whole = pl.BlockSpec((2 * PAIR, 2 * PAIR), lambda g, *s: (0, 0))
    flat = pl.BlockSpec((rows, WIDE), lambda g, *s: (0, before(g)))
    column = lambda at: pl.BlockSpec((rows, WIDE), lambda g, *s: (0, s[at][0] + before(g)))
    kept_spec = pl.BlockSpec(memory_space=pl.ANY)
    in_specs = [
        pl.BlockSpec((reps, 1, 2 * nx, LANES), lambda g, *s: (s[0][0], now(g) // 2, 0, 0)),
        pl.BlockSpec((reps,) + spots.shape[1:], lambda g, *s: (s[0][0], 0, 0)),
    ] + specs + ([kept_spec] if carries else []) + [whole, whole]
    in_specs += [pl.BlockSpec(memory_space=pl.ANY)] * len(held)
    half = jax.ShapeDtypeStruct((rows, width // 2), bf16)
    out_specs, out_shape = [flat, column(2)], [half, jax.ShapeDtypeStruct((rows, shards * width), bf16)]
    if first:
        out_specs += [flat, column(1)]
        out_shape += [half, jax.ShapeDtypeStruct((rows, width), bf16)]
    if carries:
        out_specs.append(kept_spec)
        out_shape.append(jax.ShapeDtypeStruct((1, rows, width), f32))
    at = len(scalars) + len(in_specs) - len(held)
    targets = [1, 2][: len(held)]
    return pl.pallas_call(
        functools.partial(sum_kernel, nx, topk, reps, first, carries, d * steps, cuts, len(held)),
        grid_spec=pltpu.PrefetchScalarGridSpec(
            num_scalar_prefetch=len(scalars),
            grid=(steps + 1,),
            in_specs=in_specs,
            out_specs=out_specs,
            scratch_shapes=[
                pltpu.VMEM((2, rows, WIDE), f32), pltpu.VMEM((reps, tiles, 2 * nx, LANES), f32),
                pltpu.VMEM((2, rows, WIDE), f32), pltpu.SemaphoreType.DMA((2,)), pltpu.SemaphoreType.DMA((2,)),
            ],
        ),
        out_shape=out_shape,
        input_output_aliases={at + i: t for i, t in enumerate(targets)},
        cost_estimate=pl.CostEstimate(flops=steps * 2 * 10**9, bytes_accessed=8 * 2**20, transcendentals=0),
        name="sum_part",
    )(
        *scalars, vals, spots, *[array for array, _, _ in pieces], *([kept] if carries else []),
        left_basis(basis().T), right_basis(basis()), *held,
    )


def place_kernel(count, shards, blocks, *refs):
    r, s = lax.axis_index("replica"), lax.axis_index("shard")
    far = 1 - lax.rem(r, 2)
    sems = refs[-1]
    copies = []
    for i in range(count):
        part, full = refs[i], refs[2 * count + i]
        width = part.shape[1]
        block = far if blocks[i] is None else 2 * lax.rem(s + blocks[i], shards) + far
        at = pl.ds(pl.multiple_of(block * width, width), width)
        copies.append(pltpu.make_async_copy(part, full.at[:, at], sems.at[i]))
    for copy in copies:
        copy.start()
    for copy in copies:
        copy.wait()


def put(shards, blocks, parts, fulls):
    count = len(parts)
    return pl.pallas_call(
        functools.partial(place_kernel, count, shards, blocks),
        in_specs=[pl.BlockSpec(memory_space=pl.ANY)] * (2 * count),
        out_specs=[pl.BlockSpec(memory_space=pl.ANY)] * count,
        out_shape=[jax.ShapeDtypeStruct(f.shape, f.dtype) for f in fulls],
        scratch_shapes=[pltpu.SemaphoreType.DMA((count,))],
        input_output_aliases={count + i: i for i in range(count)},
        cost_estimate=pl.CostEstimate(flops=0, bytes_accessed=2 * count * parts[0].size, transcendentals=0),
        compiler_params=pltpu.CompilerParams(vmem_limit_bytes=2**20),
        name="put",
    )(*parts, *fulls)


def per_device(reps, shards, weight, momentum, grad, positions):
    rows, width = weight.shape
    _, nx, ny, topk = positions.shape
    half = width // 2
    steps = half // WIDE
    r, s = lax.axis_index("replica"), lax.axis_index("shard")
    core = lax.rem(r, 2)
    def ring(x, d):
        return lax.ppermute(x, "shard", [(i, (i + d) % shards) for i in range(shards)])

    def across(x, bit):
        return lax.ppermute(x, "replica", [(i, i ^ bit) for i in range(reps)])

    late = 3 * steps // 8 * WIDE
    early = half - late
    mine = lax.dynamic_slice(weight, (0, core * half), (rows, early))
    others = [[ring(mine, d)] for d in range(1, shards)]

    pos = positions[0].reshape(nx, 2 * steps, LANES)
    kept, vals, spots = own_part(momentum, grad, pos, reps, shards, topk)

    if late:
        rest = lax.dynamic_slice(weight, (0, core * half + early), (rows, late))
        rest, vals = lax.optimization_barrier((rest, vals))
        for d in range(1, shards):
            others[d - 1].append(ring(rest, d))

    def scalars(of):
        return [v.reshape(1).astype(jnp.int32) for v in (of, core * steps, (of * 2 + core) * steps)]

    updated, new_weight, smooth, direction, kept_full = sum_part(
        0, shards, scalars(s), vals, spots, [(weight, True, steps)], kept, (), topk
    )
    parts = [updated]
    for d in range(1, shards):
        of = lax.rem(s - d + shards, shards)
        held = (new_weight, kept_full) if d == 1 else (new_weight,)
        out = sum_part(d, shards, scalars(of), vals, spots, [(w, False, w.shape[1] // WIDE) for w in others[d - 1]], kept, held, topk)
        updated, new_weight = out[0], out[1]
        if d == 1:
            kept_full = out[2]
        parts.append(updated)

    new_weight, direction = put(
        shards, [0, None], [across(parts[0], 1), across(smooth, 1)], [new_weight, direction]
    )
    for d in range(1, shards):
        new_weight, = put(shards, [shards - d], [across(parts[d], 1)], [new_weight])
    return (kept_full, direction, new_weight)


def solution(mesh):
    reps, shards = mesh.shape["replica"], mesh.shape["shard"]
    in_specs = (
        P(None, "shard"),
        P("replica", None, "shard"),
        P("replica", None, "shard"),
        P("replica", None, "shard", None),
    )
    out_specs = (P("replica", None, "shard"), P(None, "shard"), P())
    return jax.shard_map(
        functools.partial(per_device, reps, shards),
        mesh=mesh, in_specs=in_specs, out_specs=out_specs, check_vma=False,
    )
```

```python
import functools
import math

import jax
import jax.numpy as jnp
import numpy as np
from jax import lax
from jax.experimental import pallas as pl
from jax.experimental.pallas import tpu as pltpu
from jax.sharding import PartitionSpec as P

GROUP = 64
LANES = 128
WIDE = 256
PAIR = 128

beta_decay = 0.9
step_rate = 0.02

f32, bf16 = jnp.float32, jnp.bfloat16
MESH = pl.DeviceIdType.MESH


def basis():
    k = np.arange(GROUP, dtype=np.float64)[:, None]
    i = np.arange(GROUP, dtype=np.float64)[None, :]
    scale = np.where(k == 0, math.sqrt(1.0 / GROUP), math.sqrt(2.0 / GROUP))
    return scale * np.cos(math.pi * (2.0 * i + 1.0) * k / (2.0 * GROUP))


def halves(c):
    full = np.kron(np.eye(PAIR // GROUP), c).astype(np.float32)
    high = full.astype(bf16)
    low = (full - high.astype(np.float32)).astype(bf16)
    return high, low


def left_basis(c):
    high, low = halves(c)
    return np.block([[high, high], [low, low]])


def right_basis(c):
    high, low = halves(c)
    return np.block([[high, low], [high, low]])


def split(x):
    high = x.astype(bf16)
    return high, (x - high.astype(f32)).astype(bf16)


def dot(a, b):
    return jnp.dot(a, b, preferred_element_type=f32)


def dot_t(a, b):
    return lax.dot_general(a, b, (((1,), (1,)), ((), ())), preferred_element_type=f32)


def left(m, x):
    high, low = split(x)
    parts = []
    for at in range(0, x.shape[0], PAIR):
        both = dot(m, jnp.concatenate([high[at : at + PAIR], low[at : at + PAIR]], axis=0))
        parts.append(both[:PAIR] + both[PAIR:])
    return jnp.concatenate(parts, axis=0)


def right(x, m):
    high, low = split(x)
    rows = x.shape[0]
    ats = range(0, x.shape[1], PAIR)
    both = dot(jnp.concatenate([
        jnp.concatenate([high[:, at : at + PAIR], low[:, at : at + PAIR]], axis=1) for at in ats
    ], axis=0), m)
    both = both[:, :PAIR] + both[:, PAIR:]
    return jnp.concatenate([both[i * rows : (i + 1) * rows] for i in range(len(ats))], axis=1)


def down(rows):
    return lax.broadcasted_iota(jnp.int32, (rows, LANES), 0).astype(f32)


def lane_offset(topk):
    lane = lax.broadcasted_iota(jnp.int32, (1, LANES), 1)
    return (lane // topk * GROUP).astype(f32)


def place(pos, topk):
    a = jnp.floor(pos * (1.0 / GROUP))
    return a, pos - a * GROUP + lane_offset(topk)


def chunks_of(tiles):
    halves = [sorted({0, tiles // 2, tiles}), sorted({0, tiles // 2, tiles - 1, tiles})]
    pieces = [(h, a, b) for h in range(2) for a, b in zip(halves[h][:-1], halves[h][1:])]
    ready = [2 * (h * tiles + b) for h, _, b in pieces]
    windows = [b - a for a, b in zip(ready[:-1], ready[1:])] + [1]
    return list(zip(pieces, ready, windows))


def own_kernel(
    nx, topk, reps, shards, mom, grad, pos, lf, rt, li, ri, kept, vals, spots,
    mine, at_all, places, old, turned, place_send, place_recv, send_sem, recv_sem,
):
    g, last = pl.program_id(0), pl.num_programs(0) - 1
    tiles = mine.shape[1]
    r, s = lax.axis_index("replica"), lax.axis_index("shard")
    me = s * reps + r
    total = reps * shards

    def peer(step):
        to = lax.rem(me + step, total)
        return lax.rem(to, reps), to // reps

    def place_copy(step):
        to_r, to_s = peer(step)
        return pltpu.make_async_remote_copy(
            src_ref=places.at[lax.rem(to_r, 2)], dst_ref=spots.at[me],
            send_sem=place_send, recv_sem=place_recv, device_id=(to_r, to_s), device_id_type=MESH,
        )

    def value_copy(step, half, part):
        to = lax.rem(me // 2 + step, total // 2)
        to_s, to_r = to // (reps // 2), 2 * lax.rem(to, reps // 2) + half
        return pltpu.make_async_remote_copy(
            src_ref=mine.at[half, part], dst_ref=vals.at[me, part],
            send_sem=send_sem, recv_sem=recv_sem, device_id=(to_r, to_s), device_id_type=MESH,
        )

    def forward():
        moved = beta_decay * mom[0] + grad[0].astype(f32)
        slot = lax.rem(g, 2)
        old[slot] = moved
        turned[slot] = right(left(lf[...], moved), rt[...])

    def backward():
        u, slot = g - 1, lax.rem(g + 1, 2)
        a, b = place(at_all[pl.ds(pl.multiple_of(u * nx, nx), nx)], topk)
        rows, cols = down(GROUP), down(WIDE)
        picked, own = [], []
        for x in range(nx):
            part = turned[slot, x * GROUP : (x + 1) * GROUP]
            at_row = rows == a[x : x + 1]
            hot_a = jnp.where(at_row, 1.0, 0.0).astype(bf16)
            hot_b = jnp.where(cols == b[x : x + 1], 1.0, 0.0).astype(bf16)
            own.append(part * dot_t(hot_a, hot_b))
            high, low = split(part)
            found = dot(jnp.concatenate([high, low], axis=0), hot_b)
            found = found[:GROUP] + found[GROUP:]
            picked.append(jnp.sum(jnp.where(at_row, found, 0.0), axis=0, keepdims=True))
        rows_at = pl.ds(pl.multiple_of(lax.rem(u, 2) * nx, nx), nx)
        mine[u // (2 * tiles), lax.rem(u // 2, tiles), rows_at] = jnp.concatenate(picked, axis=0)
        kept[0] = old[slot] - right(left(li[...], jnp.concatenate(own, axis=0)), ri[...])

    @pl.when(g == 0)
    def _():
        barrier = pltpu.get_barrier_semaphore()

        @pl.loop(1, total)
        def _(step):
            pl.semaphore_signal(barrier, inc=1, device_id=peer(step), device_id_type=MESH)

        for x in range(nx):
            at_all[pl.ds(x, pos.shape[1], stride=nx)] = pos[x].astype(f32)
        each = places.shape[1]
        for half in range(2):
            places[half] = at_all[half * each : (half + 1) * each].astype(jnp.int32).astype(jnp.int16)
        forward()
        pl.semaphore_wait(barrier, total - 1)
        pltpu.make_async_copy(places.at[lax.rem(r, 2)], spots.at[me], place_recv).start()

    @pl.when((g > 0) & (g < last))
    def _():
        backward()
        forward()

    @pl.when(g == last)
    def _():
        backward()

    share = -(-(total - 1) // tiles)

    @pl.when(g < last)
    def _():
        @pl.loop(1 + g * share, jnp.minimum(1 + (g + 1) * share, total))
        def _(step):
            place_copy(step).start()

    for (half, begin, end), ready, window in chunks_of(tiles):
        each = -(-(total // 2) // window)

        @pl.when((g >= ready) & (g < ready + window))
        def _(half=half, part=pl.ds(begin, end - begin), ready=ready, each=each):
            start = (g - ready) * each

            @pl.when((g == ready) & (lax.rem(r, 2) == half))
            def _():
                pltpu.make_async_copy(mine.at[half, part], vals.at[me, part], recv_sem).start()

            @pl.when((g == ready) & (lax.rem(r, 2) != half))
            def _():
                value_copy(0, half, part).start()

            @pl.loop(jnp.maximum(start, 1), jnp.minimum(start + each, total // 2))
            def _(step):
                value_copy(step, half, part).start()

    @pl.when(g == last)
    def _():
        most = pl.ds(0, total - 1)
        pltpu.make_async_copy(spots.at[most], spots.at[most], place_send).wait()
        pltpu.make_async_copy(spots, spots, place_recv).wait()
        pltpu.make_async_copy(vals.at[most], vals.at[most], send_sem).wait()
        pltpu.make_async_copy(vals, vals, recv_sem).wait()


def own_part(mom, grad, pos, reps, shards, topk):
    _, rows, width = mom.shape
    nx = rows // GROUP
    steps = width // WIDE
    tiles = steps // 4
    total = reps * shards
    whole = pl.BlockSpec((2 * PAIR, 2 * PAIR), lambda g: (0, 0))
    now = pl.BlockSpec((1, rows, WIDE), lambda g: (0, 0, jnp.minimum(g, steps - 1)))
    dma = pltpu.SemaphoreType.DMA
    return pl.pallas_call(
        functools.partial(own_kernel, nx, topk, reps, shards),
        grid=(steps + 1,),
        in_specs=[
            now, now,
            pl.BlockSpec(pos.shape, lambda g: (0, 0, 0)),
            whole, whole, whole, whole,
        ],
        out_specs=[
            pl.BlockSpec((1, rows, WIDE), lambda g: (0, 0, jnp.maximum(g - 1, 0))),
            pl.BlockSpec(memory_space=pl.ANY),
            pl.BlockSpec(memory_space=pl.ANY),
        ],
        out_shape=[
            jax.ShapeDtypeStruct((1, rows, width), f32),
            jax.ShapeDtypeStruct((total, tiles, 2 * nx, LANES), f32),
            jax.ShapeDtypeStruct((total, steps // 2 * nx, LANES), jnp.int16),
        ],
        scratch_shapes=[
            pltpu.VMEM((2, tiles, 2 * nx, LANES), f32),
            pltpu.VMEM((steps * nx, LANES), f32),
            pltpu.VMEM((2, steps // 2 * nx, LANES), jnp.int16),
            pltpu.VMEM((2, rows, WIDE), f32), pltpu.VMEM((2, rows, WIDE), f32),
            dma, dma, dma, dma,
        ],
        compiler_params=pltpu.CompilerParams(has_side_effects=True, collective_id=0),
        name="own_part",
    )(
        mom, grad, pos,
        left_basis(basis()), right_basis(basis().T),
        left_basis(basis().T), right_basis(basis()),
    )


def regroup(tiles, topk):
    lane = lax.broadcasted_iota(jnp.int32, tiles[0].shape, 1) // topk
    each = LANES // topk
    out = []
    for y in range(each):
        mixed = tiles[y]
        for j in range(each):
            if j != y:
                moved = pltpu.roll(tiles[j], (j - y) % each * topk, axis=1)
                mixed = jnp.where(lane == j, moved, mixed)
        out.append(mixed)
    return out


def scatter(nx, topk, values, spots):
    each = LANES // topk
    rows = down(GROUP)
    fields = [[] for _ in range(each)]
    for q in range(0, len(values), each):
        mixed = zip(regroup(values[q : q + each], topk), regroup(spots[q : q + each], topk))
        for y, (value, spot) in enumerate(mixed):
            a = jnp.floor(spot * (1.0 / GROUP))
            high, low = split(value)
            fields[y].append((a, spot - a * GROUP, high.astype(f32), low.astype(f32)))
    grid = []
    for x in range(nx):
        across = []
        for y in range(each):
            ones, scaled = [], []
            for a, b, high, low in fields[y]:
                at_a = rows == a[x : x + 1]
                at_b = rows == b[x : x + 1]
                plain, chosen = (at_a, at_b) if y % 2 == 0 else (at_b, at_a)
                ones.append(jnp.where(plain, 1.0, 0.0).astype(bf16))
                scaled.append(jnp.concatenate([
                    jnp.where(chosen, high[x : x + 1], 0.0).astype(bf16),
                    jnp.where(chosen, low[x : x + 1], 0.0).astype(bf16),
                ], axis=0))
            ones, scaled = jnp.concatenate(ones, axis=1), jnp.concatenate(scaled, axis=1)
            if y % 2 == 0:
                both = dot_t(ones, scaled)
                across.append((both + pltpu.roll(both, GROUP, axis=1))[:, :GROUP])
            else:
                both = dot_t(scaled, ones)
                across.append(both[:GROUP] + both[GROUP:])
        grid.append(jnp.concatenate(across, axis=1))
    return jnp.concatenate(grid, axis=0)


def sum_kernel(nx, topk, reps, first, carries, base, cuts, held, of, near, wide, vals, spots, *refs):
    refs = list(refs)
    pieces = [refs.pop(0) for _ in cuts]
    kept_in = refs.pop(0) if carries else None
    li, ri = refs.pop(0), refs.pop(0)
    refs = refs[held:]
    updated_out, weight_out = refs.pop(0), refs.pop(0)
    smooth_out, direction_out = (refs.pop(0), refs.pop(0)) if first else (None, None)
    kept_out = refs.pop(0) if carries else None
    sums, at, hold, in_sem, out_sem = refs
    g, last = pl.program_id(0), pl.num_programs(0) - 1

    def gather():
        rows = pl.ds(pl.multiple_of(lax.rem(g, 2) * nx, nx), nx)
        tile = g // 2
        sums[lax.rem(g, 2)] = scatter(
            nx, topk, [vals[r, 0, rows] for r in range(reps)], [at[r, tile, rows] for r in range(reps)]
        )

    def finish():
        smooth = jnp.tanh(right(left(li[...], sums[lax.rem(g + 1, 2)]), ri[...]))
        weight = pieces[0][...]
        for cut, piece in zip(cuts[1:], pieces[1:]):
            weight = jnp.where(g > cut, piece[...], weight)
        updated = (weight.astype(f32) - step_rate * smooth).astype(bf16)
        updated_out[...] = updated
        weight_out[...] = updated
        if first:
            direction = smooth.astype(bf16)
            smooth_out[...] = direction
            direction_out[...] = direction

    def column(step):
        return pl.ds(pl.multiple_of((base + step) * WIDE, WIDE), WIDE)

    def bring(step):
        slot = lax.rem(step, 2)
        return pltpu.make_async_copy(kept_in.at[0, :, column(step)], hold.at[slot], in_sem.at[slot])

    def drop(step):
        slot = lax.rem(step, 2)
        return pltpu.make_async_copy(hold.at[slot], kept_out.at[0, :, column(step)], out_sem.at[slot])

    if carries:
        @pl.when((g > 1) & (g < last))
        def _():
            drop(g - 2).wait()

        @pl.when(g < last)
        def _():
            bring(g).start()

        @pl.when(g > 0)
        def _():
            bring(g - 1).wait()
            drop(g - 1).start()

    @pl.when(g == 0)
    def _():
        for r in range(reps):
            at[r] = spots[r].astype(jnp.int32).astype(f32).reshape(at.shape[1:])
        gather()

    @pl.when((g > 0) & (g < last))
    def _():
        finish()
        gather()

    @pl.when(g == last)
    def _():
        finish()
        if carries:
            drop(g - 2).wait()
            drop(g - 1).wait()


def sum_part(d, shards, scalars, vals, spots, pieces, kept, held, topk):
    rows, reps, tiles = pieces[0][0].shape[0], vals.shape[0] // shards, vals.shape[1]
    nx = rows // GROUP
    steps = 2 * tiles
    width = 2 * steps * WIDE
    first, carries = d == 0, d < 2
    now = lambda g: jnp.minimum(g, steps - 1)
    before = lambda g: jnp.maximum(g - 1, 0)
    cuts, specs = [], []
    for array, offset, count in pieces:
        cut = sum(n for _, _, n in pieces[: len(cuts)])
        cuts.append(cut)
        if offset:
            specs.append(pl.BlockSpec((rows, WIDE), lambda g, *s: (0, s[1][0] + before(g))))
        else:
            specs.append(pl.BlockSpec(
                (rows, WIDE), lambda g, *s, cut=cut, n=count: (0, jnp.clip(before(g) - cut, 0, n - 1))
            ))
    whole = pl.BlockSpec((2 * PAIR, 2 * PAIR), lambda g, *s: (0, 0))
    flat = pl.BlockSpec((rows, WIDE), lambda g, *s: (0, before(g)))
    column = lambda at: pl.BlockSpec((rows, WIDE), lambda g, *s: (0, s[at][0] + before(g)))
    kept_spec = pl.BlockSpec(memory_space=pl.ANY)
    in_specs = [
        pl.BlockSpec((reps, 1, 2 * nx, LANES), lambda g, *s: (s[0][0], now(g) // 2, 0, 0)),
        pl.BlockSpec((reps,) + spots.shape[1:], lambda g, *s: (s[0][0], 0, 0)),
    ] + specs + ([kept_spec] if carries else []) + [whole, whole]
    in_specs += [pl.BlockSpec(memory_space=pl.ANY)] * len(held)
    half = jax.ShapeDtypeStruct((rows, width // 2), bf16)
    out_specs, out_shape = [flat, column(2)], [half, jax.ShapeDtypeStruct((rows, shards * width), bf16)]
    if first:
        out_specs += [flat, column(1)]
        out_shape += [half, jax.ShapeDtypeStruct((rows, width), bf16)]
    if carries:
        out_specs.append(kept_spec)
        out_shape.append(jax.ShapeDtypeStruct((1, rows, width), f32))
    at = len(scalars) + len(in_specs) - len(held)
    targets = [1, 2][: len(held)]
    return pl.pallas_call(
        functools.partial(sum_kernel, nx, topk, reps, first, carries, d * steps, cuts, len(held)),
        grid_spec=pltpu.PrefetchScalarGridSpec(
            num_scalar_prefetch=len(scalars),
            grid=(steps + 1,),
            in_specs=in_specs,
            out_specs=out_specs,
            scratch_shapes=[
                pltpu.VMEM((2, rows, WIDE), f32), pltpu.VMEM((reps, tiles, 2 * nx, LANES), f32),
                pltpu.VMEM((2, rows, WIDE), f32), pltpu.SemaphoreType.DMA((2,)), pltpu.SemaphoreType.DMA((2,)),
            ],
        ),
        out_shape=out_shape,
        input_output_aliases={at + i: t for i, t in enumerate(targets)},
        cost_estimate=pl.CostEstimate(flops=steps * 2 * 10**9, bytes_accessed=8 * 2**20, transcendentals=0),
        name="sum_part",
    )(
        *scalars, vals, spots, *[array for array, _, _ in pieces], *([kept] if carries else []),
        left_basis(basis().T), right_basis(basis()), *held,
    )


def place_kernel(count, shards, blocks, *refs):
    r, s = lax.axis_index("replica"), lax.axis_index("shard")
    far = 1 - lax.rem(r, 2)
    sems = refs[-1]
    copies = []
    for i in range(count):
        part, full = refs[i], refs[2 * count + i]
        width = part.shape[1]
        block = far if blocks[i] is None else 2 * lax.rem(s + blocks[i], shards) + far
        at = pl.ds(pl.multiple_of(block * width, width), width)
        copies.append(pltpu.make_async_copy(part, full.at[:, at], sems.at[i]))
    for copy in copies:
        copy.start()
    for copy in copies:
        copy.wait()


def put(shards, blocks, parts, fulls):
    count = len(parts)
    return pl.pallas_call(
        functools.partial(place_kernel, count, shards, blocks),
        in_specs=[pl.BlockSpec(memory_space=pl.ANY)] * (2 * count),
        out_specs=[pl.BlockSpec(memory_space=pl.ANY)] * count,
        out_shape=[jax.ShapeDtypeStruct(f.shape, f.dtype) for f in fulls],
        scratch_shapes=[pltpu.SemaphoreType.DMA((count,))],
        input_output_aliases={count + i: i for i in range(count)},
        cost_estimate=pl.CostEstimate(flops=0, bytes_accessed=2 * count * parts[0].size, transcendentals=0),
        compiler_params=pltpu.CompilerParams(vmem_limit_bytes=2**20),
        name="put",
    )(*parts, *fulls)


def per_device(reps, shards, weight, momentum, grad, positions):
    rows, width = weight.shape
    _, nx, ny, topk = positions.shape
    half = width // 2
    steps = half // WIDE
    r, s = lax.axis_index("replica"), lax.axis_index("shard")
    core = lax.rem(r, 2)
    def ring(x, d):
        return lax.ppermute(x, "shard", [(i, (i + d) % shards) for i in range(shards)])

    def across(x, bit):
        return lax.ppermute(x, "replica", [(i, i ^ bit) for i in range(reps)])

    late = steps // 2 * WIDE
    early = half - late
    mine = lax.dynamic_slice(weight, (0, core * half), (rows, early))
    others = [[ring(mine, d)] for d in range(1, shards)]

    pos = positions[0].reshape(nx, 2 * steps, LANES)
    kept, vals, spots = own_part(momentum, grad, pos, reps, shards, topk)

    if late:
        rest = lax.dynamic_slice(weight, (0, core * half + early), (rows, late))
        rest, vals = lax.optimization_barrier((rest, vals))
        for d in range(1, shards):
            others[d - 1].append(ring(rest, d))

    def scalars(of):
        return [v.reshape(1).astype(jnp.int32) for v in (of, core * steps, (of * 2 + core) * steps)]

    updated, new_weight, smooth, direction, kept_full = sum_part(
        0, shards, scalars(s), vals, spots, [(weight, True, steps)], kept, (), topk
    )
    parts = [updated]
    for d in range(1, shards):
        of = lax.rem(s - d + shards, shards)
        held = (new_weight, kept_full) if d == 1 else (new_weight,)
        out = sum_part(d, shards, scalars(of), vals, spots, [(w, False, w.shape[1] // WIDE) for w in others[d - 1]], kept, held, topk)
        updated, new_weight = out[0], out[1]
        if d == 1:
            kept_full = out[2]
        parts.append(updated)

    new_weight, direction = put(
        shards, [0, None], [across(parts[0], 1), across(smooth, 1)], [new_weight, direction]
    )
    for d in range(1, shards):
        new_weight, = put(shards, [shards - d], [across(parts[d], 1)], [new_weight])
    return (kept_full, direction, new_weight)


def solution(mesh):
    reps, shards = mesh.shape["replica"], mesh.shape["shard"]
    in_specs = (
        P(None, "shard"),
        P("replica", None, "shard"),
        P("replica", None, "shard"),
        P("replica", None, "shard", None),
    )
    out_specs = (P("replica", None, "shard"), P(None, "shard"), P())
    return jax.shard_map(
        functools.partial(per_device, reps, shards),
        mesh=mesh, in_specs=in_specs, out_specs=out_specs, check_vma=False,
    )
```
